256 devices in a mesh: ty: 8 (over y_hi, x), tx: 32 (over y_lo, z, core).
Axes of the slice: x: 4, y: 4 (y_hi: 2, y_lo: 2; y = y_hi * 2 + y_lo), z: 8, core: 2. Of those that a mesh axis runs over, the one named last changes fastest.
Arguments:
- state: float32 [3, 1024, 16384], P(None, 'ty', 'tx'), may hold values from -6 to 6
- cut_mask: int32 [1024, 16384], P('ty', 'tx'), may hold values from 0 to 1, as said below
- fraction: int32 [1024, 16384], P('ty', 'tx'), may hold values from 256 to 1024
- neighbourhood: int32 [1024, 16384], P('ty', 'tx'), may hold values from 16 to 511, as said below
- tile_flags: int32 [8, 128], P('ty', 'tx'), may hold values from 0 to 1, as said below
- centroid_offset: float32 [2, 1024, 16384], P(None, 'ty', 'tx'), may hold values from -0.45 to 0.45
Outputs:
- redistributed: float32 [3, 1024, 16384], P(None, 'ty', 'tx')
The draws below stay inside these ranges and needn't reach their ends.
Inputs may be any that keep to these rules, and one draw needn't show every extreme that they name: Bit 3 (dy + 1) + (dx + 1) says whether the cell dy rows and dx columns away belongs to the cell's neighbourhood; bit 4 is always set, and no bit names a cell outside the grid. At the four corner cells of every block of 128 x 512 cells (rows k * 128 and k * 128 + 127, likewise for columns) every bit that names a cell inside the grid is set. `tile_flags`: the tiles at the four corners of every block of 128 x 512 cells are flagged. `cut_mask`: the four corner cells of every block of 128 x 512 cells are cut.
All inputs are finite; a program needn't handle non-finite values.
Results may differ from the reference program's by a relative error of at most 0.0003.
Values sent between devices are 32-bit elements; how exact they have to be, the bound alone decides.
No kernel may reach another device: no remote copies, remote signals or barrier semaphores. Data moves between devices by JAX's collectives and lax.ppermute only.
A program may use at most 64 MiB of HBM per device.

```python
import jax
import jax.numpy as jnp
from jax import lax

ROWS = 128
COLS = 512
TILE = 128
STEPS = 1
GRID_ROWS = 1024
GRID_COLS = 16384


def block_corners(shape_cells, block_rows, block_cols):
    row_index = lax.broadcasted_iota(jnp.int32, shape_cells, 0) % block_rows
    col_index = lax.broadcasted_iota(jnp.int32, shape_cells, 1) % block_cols
    row_edge = (row_index == 0) | (row_index == block_rows - 1)
    col_edge = (col_index == 0) | (col_index == block_cols - 1)
    return row_edge & col_edge


def draw_cut_mask(key, part):
    shape_cells = (GRID_ROWS, GRID_COLS)
    random_bits = jax.random.randint(key, shape_cells, 0, 2, dtype=jnp.int32)
    corner = block_corners(shape_cells, ROWS, COLS)
    return jnp.where(corner, 1, random_bits).astype(jnp.int32)


def draw_neighbourhood(key, part):
    shape_cells = (GRID_ROWS, GRID_COLS)
    random_bits = jax.random.randint(key, shape_cells, 0, 512, dtype=jnp.int32)
    corner = block_corners(shape_cells, ROWS, COLS)
    random_bits = jnp.where(corner, 511, random_bits).astype(jnp.int32)
    row_index = lax.broadcasted_iota(jnp.int32, shape_cells, 0)
    col_index = lax.broadcasted_iota(jnp.int32, shape_cells, 1)
    allowed = jnp.zeros(shape_cells, jnp.int32)
    bit_index = 0
    for row_step in (-1, 0, 1):
        for col_step in (-1, 0, 1):
            inside = (row_index + row_step >= 0) & (row_index + row_step < GRID_ROWS)
            inside = inside & (col_index + col_step >= 0) & (col_index + col_step < GRID_COLS)
            allowed = allowed + jnp.where(inside, 1 << bit_index, 0).astype(jnp.int32)
            bit_index = bit_index + 1
    return (random_bits | 16) & allowed


def draw_tile_flags(key, part):
    shape_tiles = (GRID_ROWS // TILE, GRID_COLS // TILE)
    scores = jax.random.randint(key, shape_tiles, 0, 1024, dtype=jnp.int32)
    col_index = lax.broadcasted_iota(jnp.int32, shape_tiles, 1)
    span_tiles = max(shape_tiles[1] - 1, 1)
    threshold = 120 + 880 * col_index // span_tiles
    corner = block_corners(shape_tiles, ROWS // TILE, COLS // TILE)
    return jnp.where(corner, 1, (scores < threshold).astype(jnp.int32)).astype(jnp.int32)


def with_ends(values, stream_key, low, high):
    longest = values.shape.index(max(values.shape))
    spots = []
    for shift in (0, 1):
        where = [jax.random.randint(jax.random.fold_in(stream_key, axis), (), 0, length) for axis, length in enumerate(values.shape)]
        where[longest] = (where[longest] + shift) % values.shape[longest]
        spots.append(tuple(where))
    return values.at[spots[0]].set(low).at[spots[1]].set(high)


def level_of(rng, extent, cuts, low, largest):
    loudness, own = 1.0, jax.random.fold_in(rng, 6)
    for dim, parts in cuts:
        draws = jnp.exp(jax.random.uniform(jax.random.fold_in(own, dim), (parts,), jnp.float32, low / len(cuts), largest / len(cuts)))
        loudness = loudness * jnp.repeat(draws, extent[dim] // parts).reshape([-1 if axis == dim else 1 for axis in range(len(extent))])
    return loudness


def gaussian(rng, dims, scale, most, shards=(), held_as=jnp.bfloat16):
    gain = level_of(rng, dims, shards, -0.22, 0.18) if shards else 1.0
    values = jax.random.normal(rng, dims, jnp.float32) * scale * gain
    return jnp.minimum(jnp.maximum(values, -most), most).astype(held_as)


def setup_inputs(seed: int = 0) -> dict:
    keys = jax.random.split(jax.random.key(seed), 7)
    return {
        "state": gaussian(keys[0], (3, GRID_ROWS, GRID_COLS), 1.0, 6.0, ((1, 8), (2, 32)), jnp.float32),
        "cut_mask": draw_cut_mask(jax.random.fold_in(keys[6], 71), 0),
        "fraction": with_ends(jax.random.randint(keys[2], (GRID_ROWS, GRID_COLS), 256, 1025), jax.random.fold_in(keys[2], 1), 256, 1024).astype(jnp.int32),
        "neighbourhood": draw_neighbourhood(jax.random.fold_in(keys[6], 71), 0),
        "tile_flags": draw_tile_flags(jax.random.fold_in(keys[6], 71), 0),
        "centroid_offset": jnp.clip(jax.random.uniform(keys[5], (2, GRID_ROWS, GRID_COLS), jnp.float32, -0.45, 0.45) * level_of(keys[5], (2, GRID_ROWS, GRID_COLS), ((1, 8), (2, 32)), -0.4, 0.0), -0.45, 0.45),
    }


courant = 0.1
cell_offsets = [(row_step, col_step) for row_step in (-1, 0, 1) for col_step in (-1, 0, 1)]


def window(padded, row_step, col_step):
    height = padded.shape[-2] - 2
    width = padded.shape[-1] - 2
    return padded[..., 1 + row_step:1 + row_step + height, 1 + col_step:1 + col_step + width]


def spread(values, row_step, col_step):
    widths = [(0, 0)] * (values.ndim - 2) + [(1 + row_step, 1 - row_step), (1 + col_step, 1 - col_step)]
    return jnp.pad(values, widths)


def pad_cells(values):
    widths = [(0, 0)] * (values.ndim - 2) + [(1, 1), (1, 1)]
    return jnp.pad(values, widths)


def members_of(code_bits, active):
    result = []
    for bit_index in range(9):
        bit_value = jnp.right_shift(code_bits, bit_index) & 1
        centre_value = 1 if bit_index == 4 else 0
        result.append(jnp.where(active > 0, bit_value, centre_value).astype(jnp.float32))
    return result


def advance(padded, inv_volume):
    centre = window(padded, 0, 0)
    eastern = window(padded, 0, 1)
    western = window(padded, 0, -1)
    northern = window(padded, 1, 0)
    southern = window(padded, -1, 0)
    mass_flux = 0.5 * ((eastern[1] - western[1]) + (northern[2] - southern[2]))
    xmom_flux = 0.5 * (eastern[0] - western[0])
    ymom_flux = 0.5 * (northern[0] - southern[0])
    smoothing = eastern + western + northern + southern - 4.0 * centre
    divergence = jnp.stack([mass_flux, xmom_flux, ymom_flux]) - 0.5 * smoothing
    return centre - courant * inv_volume * divergence


def geometry(members, share_pad, offset_pad):
    total = 0.0
    sum_x = 0.0
    sum_y = 0.0
    for bit_index, (row_step, col_step) in enumerate(cell_offsets):
        weight = members[bit_index] * window(share_pad, row_step, col_step)
        total = total + weight
        sum_x = sum_x + weight * (col_step + window(offset_pad[0], row_step, col_step))
        sum_y = sum_y + weight * (row_step + window(offset_pad[1], row_step, col_step))
    return total, jnp.stack([sum_x / total, sum_y / total])


def averages(members, share_pad, star_pad, total):
    summed = 0.0
    for bit_index, (row_step, col_step) in enumerate(cell_offsets):
        weight = members[bit_index] * window(share_pad, row_step, col_step)
        summed = summed + weight * window(star_pad, row_step, col_step)
    return summed / total


def slopes(average, average_pad, centroid, centroid_pad):
    moment_xx = 1.0
    moment_xy = 0.0
    moment_yy = 1.0
    right_x = 0.0
    right_y = 0.0
    for row_step, col_step in cell_offsets:
        if row_step == 0 and col_step == 0:
            continue
        apart_x = col_step + window(centroid_pad[0], row_step, col_step) - centroid[0]
        apart_y = row_step + window(centroid_pad[1], row_step, col_step) - centroid[1]
        change = window(average_pad, row_step, col_step) - average
        moment_xx = moment_xx + apart_x * apart_x
        moment_xy = moment_xy + apart_x * apart_y
        moment_yy = moment_yy + apart_y * apart_y
        right_x = right_x + apart_x * change
        right_y = right_y + apart_y * change
    determinant = moment_xx * moment_yy - moment_xy * moment_xy
    slope_x = (moment_yy * right_x - moment_xy * right_y) / determinant
    slope_y = (moment_xx * right_y - moment_xy * right_x) / determinant
    return slope_x, slope_y


def pushed(members, kappa_cell, average, slope_x, slope_y, centroid, offset_pad):
    extended = 0.0
    for bit_index, (row_step, col_step) in enumerate(cell_offsets):
        toward_x = col_step + window(offset_pad[0], row_step, col_step) - centroid[0]
        toward_y = row_step + window(offset_pad[1], row_step, col_step) - centroid[1]
        value = (members[bit_index] * kappa_cell) * (average + slope_x * toward_x + slope_y * toward_y)
        extended = extended + spread(value, row_step, col_step)
    return extended


def reference(state, cut_mask, fraction, neighbourhood, tile_flags, centroid_offset):
    flag_cells = jnp.repeat(jnp.repeat(tile_flags, TILE, axis=0), TILE, axis=1)
    active = flag_cells * cut_mask
    kappa_cell = jnp.where(active > 0, fraction.astype(jnp.float32) * (1.0 / 1024.0), 1.0).astype(jnp.float32)
    inv_volume = 1.0 / kappa_cell
    offset_cell = centroid_offset * active.astype(jnp.float32)
    members = members_of(neighbourhood, active)
    gathered = 0.0
    for bit_index, (row_step, col_step) in enumerate(cell_offsets):
        gathered = gathered + spread(members[bit_index] * kappa_cell, row_step, col_step)
    coverage = gathered[1:-1, 1:-1]
    share_cell = kappa_cell / coverage
    share_pad = pad_cells(share_cell)
    offset_pad = pad_cells(offset_cell)
    total, centroid = geometry(members, share_pad, offset_pad)
    centroid_pad = pad_cells(centroid)

    def one_step(step_index, current):
        star = advance(pad_cells(current), inv_volume)
        average = averages(members, share_pad, pad_cells(star), total)
        slope_x, slope_y = slopes(average, pad_cells(average), centroid, centroid_pad)
        extended = pushed(members, kappa_cell, average, slope_x, slope_y, centroid, offset_pad)
        return extended[:, 1:-1, 1:-1] / coverage

    return lax.fori_loop(0, STEPS, one_step, state)
```

```python
import functools

import jax
import jax.numpy as jnp
from jax import lax
from jax.experimental import pallas as pl
from jax.experimental.pallas import tpu as pltpu
from jax.sharding import PartitionSpec as P

DEPTH = 4
LANES = 128
FIELDS = 7
PACKED = 4 * FIELDS
VMEM_LIMIT = 56 * 1024 * 1024

courant = 0.1


def paired(value, axis, other, first):
    length, width = lax.axis_size(axis), lax.axis_size(other)
    pairs = []
    for i in range(length):
        for j in range(width):
            mate = (i + 1 if (i - first) % 2 == 0 else i - 1, j)
            if not 0 <= mate[0] < length:
                mate = (i, j ^ 1)
            here = i * width + j
            there = mate[0] * width + mate[1]
            pairs.append((here, there))
    if axis == "tx":
        swap = lambda k: (k % width) * length + k // width
        pairs = [(swap(a), swap(b)) for a, b in pairs]
    return lax.ppermute(value, ("ty", "tx"), sorted(pairs))


def lane_index():
    return lax.broadcasted_iota(jnp.int32, (8, LANES), 1)


def from_west(values, west, lane):
    return [
        pltpu.roll(jnp.where(lane == LANES - 1, values[west[t]], values[t]), 1, 1)
        for t in range(len(values))
    ]


def from_east(values, east, lane):
    return [
        pltpu.roll(jnp.where(lane == 0, values[east[t]], values[t]), LANES - 1, 1)
        for t in range(len(values))
    ]


def inverse(value):
    guess = pl.reciprocal(value, approx=True)
    return guess * (2.0 - value * guess)


def store_members(mk, code, kappa, t, rows, order):
    for b in range(9):
        held = (code & (1 << order[b])) != 0
        mk[b, t, rows, :] = jnp.where(held, kappa, 0.0)


plain_order = (0, 1, 2, 3, 4, 5, 6, 7, 8)
swapped_order = (0, 3, 6, 1, 4, 7, 2, 5, 8)


class Fields:
    def __init__(self, mk, raw, rc, gath, cent, horiz, push):
        self.mk, self.raw, self.rc = mk, raw, rc
        self.gath, self.cent, self.horiz, self.push = gath, cent, horiz, push

    @staticmethod
    def shapes(tiles, rows):
        shape = lambda n: pltpu.VMEM((n, tiles, rows, LANES), jnp.float32)
        return [shape(9), shape(6), shape(1), shape(18), shape(5), shape(14), shape(9)]


def at(ref, i, t, base, step=0):
    return ref[i, t, pl.ds(base + step, 8), :]


def stage_share(s, tiles, west, east, base):
    lane = lane_index()
    n = len(tiles)
    sums = []
    for dx in (-1, 0, 1):
        group = []
        for t in tiles:
            total = at(s.mk, 4 + dx, t, base)
            total = total + at(s.mk, 1 + dx, t, base, 1)
            total = total + at(s.mk, 7 + dx, t, base, -1)
            group.append(total)
        sums.append(group)
    low = from_east(sums[0], east, lane)
    high = from_west(sums[2], west, lane)
    centre = [[at(s.raw, 3 + f, t, base) for t in tiles] for f in range(3)]
    easts = [from_east(c, east, lane) for c in centre]
    wests = [from_west(c, west, lane) for c in centre]
    outs = [[] for _ in range(6)]
    for k, t in enumerate(tiles):
        coverage = jnp.maximum(sums[1][k] + low[k] + high[k], 0.125)
        rc = inverse(coverage)
        s.rc[0, t, pl.ds(base, 8), :] = rc
        share = at(s.raw, 0, t, base) * rc
        rate = (0.5 * courant) * rc
        keep = share - 4.0 * rate
        c = [centre[f][k] for f in range(3)]
        e = [easts[f][k] for f in range(3)]
        w = [wests[f][k] for f in range(3)]
        north = [at(s.raw, 3 + f, t, base, 1) for f in range(3)]
        south = [at(s.raw, 3 + f, t, base, -1) for f in range(3)]
        flux = [(e[1] - w[1]) + (north[2] - south[2]), e[0] - w[0], north[0] - south[0]]
        outs[0].append(share)
        outs[1].append(share * at(s.raw, 1, t, base))
        outs[2].append(share * at(s.raw, 2, t, base))
        for f in range(3):
            around = (e[f] + w[f]) + (north[f] + south[f])
            outs[3 + f].append(keep * c[f] - rate * (flux[f] - around))
    for f in range(6):
        w = from_west(outs[f], west, lane)
        e = from_east(outs[f], east, lane)
        for k, t in enumerate(tiles):
            s.gath[3 * f, t, pl.ds(base, 8), :] = w[k]
            s.gath[3 * f + 1, t, pl.ds(base, 8), :] = outs[f][k]
            s.gath[3 * f + 2, t, pl.ds(base, 8), :] = e[k]


def stage_average(s, tiles, west, east, base):
    lane = lane_index()
    results = [[] for _ in range(5)]
    for t in tiles:
        weight = {}
        for dy in (-1, 0, 1):
            for dx in (-1, 0, 1):
                member = at(s.mk, 3 * (dy + 1) + dx + 1, t, base)
                weight[dy, dx] = (member, member * at(s.gath, 1 + dx, t, base, dy))
        cols = [weight[-1, d][1] + weight[0, d][1] + weight[1, d][1] for d in (-1, 0, 1)]
        total = cols[0] + cols[1] + cols[2]
        upper = weight[1, -1][1] + weight[1, 0][1] + weight[1, 1][1]
        lower = weight[-1, -1][1] + weight[-1, 0][1] + weight[-1, 1][1]
        sums = [cols[2] - cols[0], upper - lower, None, None, None]
        for f in range(5):
            for dy in (-1, 0, 1):
                for dx in (-1, 0, 1):
                    term = weight[dy, dx][0] * at(s.gath, 3 * (f + 1) + 1 + dx, t, base, dy)
                    sums[f] = term if sums[f] is None else sums[f] + term
        inv = inverse(jnp.maximum(total, 1e-3))
        for f in range(5):
            value = sums[f] * inv
            s.cent[f, t, pl.ds(base, 8), :] = value
            results[f].append(value)
    w = [from_west(r, west, lane) for r in results]
    e = [from_east(r, east, lane) for r in results]
    for k, t in enumerate(tiles):
        x = [w[0][k] - 1.0, results[0][k], e[0][k] + 1.0]
        v = [w[1][k], results[1][k], e[1][k]]
        a = [[w[2 + f][k], results[2 + f][k], e[2 + f][k]] for f in range(3)]
        add3 = lambda p: p[0] + p[1] + p[2]
        dot3 = lambda p, q: p[0] * q[0] + p[1] * q[1] + p[2] * q[2]
        made = [add3(x), add3(v), dot3(x, x), dot3(x, v), dot3(v, v)]
        made += [add3(a[f]) for f in range(3)]
        made += [dot3(x, a[f]) for f in range(3)]
        made += [dot3(v, a[f]) for f in range(3)]
        for i, value in enumerate(made):
            s.horiz[i, t, pl.ds(base, 8), :] = value


def stage_slope(s, tiles, base):
    for t in tiles:
        rows = lambda i: [at(s.horiz, i, t, base, d) for d in (-1, 0, 1)]
        add3 = lambda p: p[0] + p[1] + p[2]
        u, v = at(s.cent, 0, t, base), at(s.cent, 1, t, base)
        hx, hv = rows(0), rows(1)
        sum_x, sum_y = add3(hx), add3(hv)
        sum_xx = add3(rows(2)) + 1.0
        sum_xy = add3(rows(3)) + (hx[2] - hx[0])
        sum_yy = add3(rows(4)) + (2.0 * (hv[2] - hv[0]) + 7.0)
        mean_x = sum_x - 9.0 * u
        mean_y = sum_y - 9.0 * v
        moment_xx = sum_xx - u * (sum_x + mean_x)
        moment_yy = sum_yy - v * (sum_y + mean_y)
        moment_xy = sum_xy - u * sum_y - v * mean_x
        inv = inverse(moment_xx * moment_yy - moment_xy * moment_xy)
        moment_xx = moment_xx * inv
        moment_yy = moment_yy * inv
        moment_xy = moment_xy * inv
        for f in range(3):
            average = at(s.cent, 2 + f, t, base)
            ha = rows(5 + f)
            sum_a = add3(ha)
            right_x = add3(rows(8 + f)) - u * sum_a - average * mean_x
            right_y = add3(rows(11 + f)) + (ha[2] - ha[0]) - v * sum_a - average * mean_y
            slope_x = moment_yy * right_x - moment_xy * right_y
            slope_y = moment_xx * right_y - moment_xy * right_x
            s.push[f, t, pl.ds(base, 8), :] = average - slope_x * u - slope_y * v
            s.push[3 + f, t, pl.ds(base, 8), :] = slope_x
            s.push[6 + f, t, pl.ds(base, 8), :] = slope_y


def stage_push(s, tiles, west, east, base):
    lane = lane_index()
    off = [[at(s.raw, 1 + i, t, base) for t in tiles] for i in range(2)]
    west_off = [from_west(o, west, lane) for o in off]
    east_off = [from_east(o, east, lane) for o in off]
    groups = []
    for dx in (-1, 0, 1):
        seen = (west_off, off, east_off)[dx + 1]
        group = [[] for _ in range(3)]
        for k, t in enumerate(tiles):
            x = seen[0][k] + float(dx) if dx else seen[0][k]
            totals = [None] * 3
            for dy in (-1, 0, 1):
                y = seen[1][k] + float(dy) if dy else seen[1][k]
                member = at(s.mk, 3 * (dy + 1) + dx + 1, t, base, -dy)
                for f in range(3):
                    plane = at(s.push, f, t, base, -dy)
                    plane = plane + at(s.push, 3 + f, t, base, -dy) * x
                    plane = plane + at(s.push, 6 + f, t, base, -dy) * y
                    term = member * plane
                    totals[f] = term if totals[f] is None else totals[f] + term
            for f in range(3):
                group[f].append(totals[f])
        groups.append(group)
    results = []
    for f in range(3):
        low = from_east(groups[0][f], east, lane)
        high = from_west(groups[2][f], west, lane)
        results.append(
            [
                (groups[1][f][k] + low[k] + high[k]) * at(s.rc, 0, t, base)
                for k, t in enumerate(tiles)
            ]
        )
    return results


def start_all(copies):
    for copy in copies:
        copy.start()
    for copy in copies:
        copy.wait()


def pack_kernel(
    state, cut, fraction, code, flags, offset, s0, s1, p0, p1, own_rows, own_cols,
    st_r, ct_r, fr_r, cd_r, of_r, st_c, ct_c, fr_c, cd_c, of_c, mix, sem,
):
    rows = state.shape[1]
    cols = state.shape[2]
    copies = []
    for i, row in enumerate((0, rows - 8)):
        rs = pl.ds(row, 8)
        copies += [
            pltpu.make_async_copy(state.at[:, rs, :], st_r.at[i], sem.at[0, i]),
            pltpu.make_async_copy(cut.at[rs, :], ct_r.at[i], sem.at[1, i]),
            pltpu.make_async_copy(fraction.at[rs, :], fr_r.at[i], sem.at[2, i]),
            pltpu.make_async_copy(code.at[rs, :], cd_r.at[i], sem.at[3, i]),
            pltpu.make_async_copy(offset.at[:, rs, :], of_r.at[i], sem.at[4, i]),
        ]
    for i, col in enumerate((0, cols - LANES)):
        cs = pl.ds(col, LANES)
        copies += [
            pltpu.make_async_copy(state.at[:, :, cs], st_c.at[i], sem.at[5, i]),
            pltpu.make_async_copy(cut.at[:, cs], ct_c.at[i], sem.at[6, i]),
            pltpu.make_async_copy(fraction.at[:, cs], fr_c.at[i], sem.at[7, i]),
            pltpu.make_async_copy(code.at[:, cs], cd_c.at[i], sem.at[8, i]),
            pltpu.make_async_copy(offset.at[:, :, cs], of_c.at[i], sem.at[9, i]),
        ]
    start_all(copies)
    ntile = cols // LANES
    even_y = lax.rem(lax.axis_index("ty"), 2) == 0
    even_x = lax.rem(lax.axis_index("tx"), 2) == 0

    def fields(st, ct, fr, cd, of, flag):
        active = ct > (1 - flag)
        return [
            jnp.where(active, cd, 16).astype(jnp.float32),
            jnp.where(active, fr.astype(jnp.float32) * (1.0 / 1024.0), 1.0),
            jnp.where(active, of[0], 0.0),
            jnp.where(active, of[1], 0.0),
            st[0],
            st[1],
            st[2],
        ]

    mids = {}
    for t in range(ntile):
        ls = pl.ds(t * LANES, LANES)
        made = []
        for i in range(2):
            got = fields(
                st_r[i, :, :, ls], ct_r[i, :, ls], fr_r[i, :, ls], cd_r[i, :, ls], of_r[i, :, :, ls],
                flags[0, t],
            )
            for f in range(FIELDS):
                own_rows[i, f, :, ls] = got[f]
            made.append(got)
        for f in range(FIELDS):
            top = made[0][f][0:4]
            bottom = made[1][f][4:8]
            s0[pl.ds(4 * f, 4), ls] = jnp.where(even_y, bottom, top)
            s1[pl.ds(4 * f, 4), ls] = jnp.where(even_y, top, bottom)
        if t in (0, ntile - 1):
            side = 0 if t == 0 else 1
            mids[side] = made
    for side, t in enumerate((0, ntile - 1)):
        got = fields(st_c[side], ct_c[side], fr_c[side], cd_c[side], of_c[side], flags[0, t])
        first = 0 if side == 0 else LANES - 8
        for f in range(FIELDS):
            own_cols[side, f, :, :] = got[f].T[first : first + 8, :]
    for f in range(FIELDS):
        left = own_cols[0, f, 0:4, :]
        right = own_cols[1, f, 4:8, :]
        rs = pl.ds(4 * f, 4)
        p0[rs, 0:LANES] = jnp.where(even_x, right, left)
        p1[rs, 0:LANES] = jnp.where(even_x, left, right)
        for side in range(2):
            first = 0 if side == 0 else LANES - 4
            near, far = mids[side][0][f], mids[side][1][f]
            for g, piece in ((1, near[0:4]), (2, near[4:8]), (3, far[0:4]), (4, far[4:8])):
                mix[side, g, rs, :] = pltpu.roll(piece, (4 * g - first) % LANES, 1)
    lane = lax.broadcasted_iota(jnp.int32, (PACKED, LANES), 1)
    parts = []
    for side in range(2):
        total = jnp.zeros((PACKED, LANES), jnp.float32)
        for g in range(1, 5):
            here = (lane >= 4 * g) & (lane < 4 * g + 4)
            total = jnp.where(here, mix[side, g, 0:PACKED, :], total)
        parts.append(total)
    p0[:, LANES:] = jnp.where(even_x, parts[1], parts[0])
    p1[:, LANES:] = jnp.where(even_x, parts[0], parts[1])


def pack(state, cut, fraction, code, flags, offset):
    rows, cols = cut.shape
    any_spec = pl.BlockSpec(memory_space=pl.ANY)
    f32, i32 = jnp.float32, jnp.int32
    strip = lambda *s: jax.ShapeDtypeStruct(s, f32)
    return pl.pallas_call(
        pack_kernel,
        out_shape=(
            strip(PACKED, cols), strip(PACKED, cols), strip(PACKED, 2 * LANES), strip(PACKED, 2 * LANES),
            strip(2, FIELDS, 8, cols), strip(2, FIELDS, 8, rows),
        ),
        in_specs=[any_spec] * 4 + [pl.BlockSpec(memory_space=pltpu.SMEM), any_spec],
        scratch_shapes=[
            pltpu.VMEM((2, 3, 8, cols), f32),
            pltpu.VMEM((2, 8, cols), i32),
            pltpu.VMEM((2, 8, cols), i32),
            pltpu.VMEM((2, 8, cols), i32),
            pltpu.VMEM((2, 2, 8, cols), f32),
            pltpu.VMEM((2, 3, rows, LANES), f32),
            pltpu.VMEM((2, rows, LANES), i32),
            pltpu.VMEM((2, rows, LANES), i32),
            pltpu.VMEM((2, rows, LANES), i32),
            pltpu.VMEM((2, 2, rows, LANES), f32),
            pltpu.VMEM((2, 5, 32, LANES), f32),
            pltpu.SemaphoreType.DMA((10, 2)),
        ],
        compiler_params=pltpu.CompilerParams(vmem_limit_bytes=VMEM_LIMIT),
        name="pack",
    )(state, cut, fraction, code, flags, offset)


def inner_kernel(state, cut, fraction, code, flags, offset, out, ct, fr, cd, *rest):
    s = Fields(*rest[:7])
    res, sem = rest[7:]
    rows = cut.shape[0]
    ntile = cut.shape[1] // LANES
    tiles = list(range(ntile))
    west = [(t - 1) % ntile for t in tiles]
    east = [(t + 1) % ntile for t in tiles]
    own = pl.ds(8, rows)
    copies = []
    for t in tiles:
        ls = pl.ds(t * LANES, LANES)
        copies += [
            pltpu.make_async_copy(cut.at[:, ls], ct.at[t], sem.at[0, t]),
            pltpu.make_async_copy(fraction.at[:, ls], fr.at[t], sem.at[1, t]),
            pltpu.make_async_copy(code.at[:, ls], cd.at[t], sem.at[2, t]),
        ]
        for i in range(2):
            copies.append(
                pltpu.make_async_copy(offset.at[i, :, ls], s.raw.at[1 + i, t, own, :], sem.at[3 + i, t])
            )
        for f in range(3):
            copies.append(
                pltpu.make_async_copy(state.at[f, :, ls], s.raw.at[3 + f, t, own, :], sem.at[5 + f, t])
            )
    start_all(copies)
    ntr = rows // 8

    def prepare(k, carry):
        src = pl.ds(pl.multiple_of(8 * k, 8), 8)
        dst = pl.ds(pl.multiple_of(8 * k + 8, 8), 8)
        for t in tiles:
            active = ct[t, src, :] > (1 - flags[0, t])
            codes = jnp.where(active, cd[t, src, :], 16)
            kappa = jnp.where(active, fr[t, src, :].astype(jnp.float32) * (1.0 / 1024.0), 1.0)
            s.raw[0, t, dst, :] = kappa
            for i in range(2):
                s.raw[1 + i, t, dst, :] = jnp.where(active, s.raw[1 + i, t, dst, :], 0.0)
            store_members(s.mk, codes, kappa, t, dst, plain_order)
        return carry

    lax.fori_loop(0, ntr, prepare, 0)

    def share(k, carry):
        stage_share(s, tiles, west, east, 8 * k + 8)
        return carry

    def average(k, carry):
        stage_average(s, tiles, west, east, 8 * k + 8)
        return carry

    def slope(k, carry):
        stage_slope(s, tiles, 8 * k + 8)
        return carry

    def push(k, carry):
        made = stage_push(s, tiles, west, east, 8 * k + 8)
        for f in range(3):
            for t in tiles:
                res[f, pl.ds(pl.multiple_of(8 * k, 8), 8), pl.ds(t * LANES, LANES)] = made[f][t]
        return carry

    for step in (share, average, slope, push):
        lax.fori_loop(0, ntr, step, 0)
    copy = pltpu.make_async_copy(res, out, sem.at[8, 0])
    copy.start()
    copy.wait()


def inner(state, cut, fraction, code, flags, offset):
    rows, cols = cut.shape
    ntile = cols // LANES
    any_spec = pl.BlockSpec(memory_space=pl.ANY)
    ints = pltpu.VMEM((ntile, rows, LANES), jnp.int32)
    return pl.pallas_call(
        inner_kernel,
        out_shape=jax.ShapeDtypeStruct(state.shape, jnp.float32),
        in_specs=[any_spec] * 4 + [pl.BlockSpec(memory_space=pltpu.SMEM), any_spec],
        out_specs=any_spec,
        scratch_shapes=[ints, ints, ints]
        + Fields.shapes(ntile, rows + 16)
        + [pltpu.VMEM(state.shape, jnp.float32), pltpu.SemaphoreType.DMA((9, ntile))],
        compiler_params=pltpu.CompilerParams(vmem_limit_bytes=VMEM_LIMIT),
        cost_estimate=pl.CostEstimate(flops=60_000_000, transcendentals=0, bytes_accessed=3_000_000),
        name="inner",
    )(state, cut, fraction, code, flags, offset)


swap_fields = (0, 1, 3, 2, 4, 6, 5)


def rim_kernel(h0, h1, c0, c1, own_rows, own_cols, base_ref, inner_out, out, wide, *rest):
    s = Fields(*rest[:7])
    res, turn, edge_c, edge_r, sem = rest[7:]
    rows, cols = inner_out.shape[1:]
    ntile = cols // LANES
    reads = []
    for i, col in enumerate((0, cols - LANES)):
        reads.append(
            pltpu.make_async_copy(inner_out.at[:, :, pl.ds(col, LANES)], edge_c.at[i], sem.at[0, i])
        )
    for i, row in enumerate((0, rows - 8)):
        reads.append(
            pltpu.make_async_copy(
                inner_out.at[:, pl.ds(row, 8), pl.ds(LANES, cols - 2 * LANES)], edge_r.at[i], sem.at[1, i]
            )
        )
    for copy in reads:
        copy.start()
    iy, ix = lax.axis_index("ty"), lax.axis_index("tx")
    even_y, even_x = lax.rem(iy, 2) == 0, lax.rem(ix, 2) == 0
    have_top, have_bottom = iy > 0, iy < lax.axis_size("ty") - 1
    have_left, have_right = ix > 0, ix < lax.axis_size("tx") - 1
    group = ntile + 1
    top, bottom, left, right = 0, group, 2 * group, 2 * group + 1
    zero4 = jnp.zeros((4, LANES), jnp.float32)
    halo = lambda even, a, b, have: jnp.where(have, jnp.where(even, a, b), zero4)
    for f in range(FIELDS):
        rs = pl.ds(4 * f, 4)
        for t in range(ntile):
            ls = pl.ds(t * LANES, LANES)
            wide[f, top + t, 0:4, :] = halo(even_y, h1[rs, ls], h0[rs, ls], have_top)
            wide[f, top + t, 4:12, :] = own_rows[0, f, :, ls]
            wide[f, bottom + t, 0:8, :] = own_rows[1, f, :, ls]
            wide[f, bottom + t, 8:12, :] = halo(even_y, h0[rs, ls], h1[rs, ls], have_bottom)
        fe = swap_fields[f]
        wide[fe, left, 0:4, :] = halo(even_x, c1[rs, 0:LANES], c0[rs, 0:LANES], have_left)
        wide[fe, left, 4:12, :] = own_cols[0, f, :, :]
        wide[fe, right, 0:8, :] = own_cols[1, f, :, :]
        wide[fe, right, 8:12, :] = halo(even_x, c0[rs, 0:LANES], c1[rs, 0:LANES], have_right)
    lane = lax.broadcasted_iota(jnp.int32, (PACKED, LANES), 1)
    none = jnp.zeros((PACKED, LANES), jnp.float32)
    a, b = c0[:, LANES:], c1[:, LANES:]
    from_left = jnp.where(have_left, jnp.where(even_x, b, a), none)
    from_right = jnp.where(have_right, jnp.where(even_x, a, b), none)
    for g in range(6):
        l = pltpu.roll(from_left, LANES - 4 - 4 * g, 1)
        r = pltpu.roll(from_right, (LANES - 4 * g) % LANES, 1)
        both = jnp.where(lane < 4, r, jnp.where(lane >= LANES - 4, l, 0.0))
        strip, first = ((top, 4 * g) if g < 3 else (bottom, 4 * (g - 3)))
        for f in range(FIELDS):
            wide[f, strip + ntile, first : first + 4, :] = both[4 * f : 4 * f + 4, :]

    tiles = list(range(2 * group + 2))
    west, east = list(tiles), list(tiles)
    for first in (top, bottom):
        for t in range(group):
            west[first + t] = first + (t - 1) % group
            east[first + t] = first + (t + 1) % group
    base = base_ref[0]
    for t in tiles:
        order = plain_order if t < left else swapped_order
        for r in range(2):
            rs = pl.ds(8 * r, 8)
            kappa = wide[1, t, rs, :]
            store_members(s.mk, wide[0, t, rs, :].astype(jnp.int32), kappa, t, rs, order)
            s.raw[0, t, rs, :] = kappa
            for f in range(2, FIELDS):
                s.raw[f - 1, t, rs, :] = wide[f, t, rs, :]
    for first in (0, 5, 10):
        pick = tiles[first : first + 5]
        w = [west[t] - first for t in pick]
        e = [east[t] - first for t in pick]
        stage_share(s, pick, w, e, base + 1)
        stage_share(s, pick, w, e, base + 9)
        stage_average(s, pick, w, e, base + 2)
        stage_slope(s, pick, base + 3)
        made = stage_push(s, pick, w, e, base + 4)
        for f in range(3):
            for k, t in enumerate(pick):
                res[f, t, :, :] = made[f][k]
    for copy in reads:
        copy.wait()
    turn[...] = jnp.zeros_like(turn)
    for f in range(3):
        fe = (0, 2, 1)[f]
        turn[pl.ds(4 * f, 4), :] = res[fe, left, 0:4, :]
        turn[pl.ds(16 + 4 * f, 4), :] = res[fe, right, 0:4, :]
    back = turn[...].T
    lane = lax.broadcasted_iota(jnp.int32, (rows, LANES), 1)
    for f in range(3):
        edge_c[0, f] = jnp.where(lane < 4, pltpu.roll(back, (LANES - 4 * f) % LANES, 1), edge_c[0, f])
        edge_c[1, f] = jnp.where(
            lane >= LANES - 4, pltpu.roll(back, LANES - 4 - 16 - 4 * f, 1), edge_c[1, f]
        )
        for i, t in enumerate((0, ntile - 1)):
            edge_c[i, f, 0:4, :] = res[f, top + t, 0:4, :]
            edge_c[i, f, rows - 4 : rows, :] = res[f, bottom + t, 0:4, :]
        for t in range(1, ntile - 1):
            ls = pl.ds((t - 1) * LANES, LANES)
            edge_r[0, f, 0:4, ls] = res[f, top + t, 0:4, :]
            edge_r[1, f, 4:8, ls] = res[f, bottom + t, 0:4, :]
    writes = []
    for i, col in enumerate((0, cols - LANES)):
        writes.append(
            pltpu.make_async_copy(edge_c.at[i], out.at[:, :, pl.ds(col, LANES)], sem.at[0, i])
        )
    for i, row in enumerate((0, rows - 8)):
        writes.append(
            pltpu.make_async_copy(
                edge_r.at[i], out.at[:, pl.ds(row, 8), pl.ds(LANES, cols - 2 * LANES)], sem.at[1, i]
            )
        )
    start_all(writes)


def rim(h0, h1, c0, c1, own_rows, own_cols, inner_out):
    rows, cols = inner_out.shape[1:]
    ntile = cols // LANES
    tiles = 2 * (ntile + 1) + 2
    any_spec = pl.BlockSpec(memory_space=pl.ANY)
    vmem = pl.BlockSpec(memory_space=pltpu.VMEM)
    f32 = jnp.float32
    return pl.pallas_call(
        rim_kernel,
        out_shape=jax.ShapeDtypeStruct(inner_out.shape, f32),
        in_specs=[vmem] * 6 + [pl.BlockSpec(memory_space=pltpu.SMEM), any_spec],
        out_specs=any_spec,
        input_output_aliases={7: 0},
        scratch_shapes=[pltpu.VMEM((FIELDS, tiles, 16, LANES), f32)]
        + Fields.shapes(tiles, 24)
        + [
            pltpu.VMEM((3, tiles, 8, LANES), f32),
            pltpu.VMEM((LANES, LANES), f32),
            pltpu.VMEM((2, 3, rows, LANES), f32),
            pltpu.VMEM((2, 3, 8, cols - 2 * LANES), f32),
            pltpu.SemaphoreType.DMA((2, 2)),
        ],
        compiler_params=pltpu.CompilerParams(vmem_limit_bytes=VMEM_LIMIT),
        cost_estimate=pl.CostEstimate(flops=10_000_000, transcendentals=0, bytes_accessed=1_000_000),
        name="rim",
    )(h0, h1, c0, c1, own_rows, own_cols, jnp.zeros((1,), jnp.int32), inner_out)


def with_corners(payload, right_side, top, bottom):
    cols = top.shape[1]
    pick = lambda h: jnp.where(right_side, h[:, cols - 4 :], h[:, :4])
    above = jnp.pad(pick(top), ((0, 0), (LANES, LANES - 4)))
    below = jnp.pad(pick(bottom), ((0, 0), (LANES + 20, LANES - 24)))
    return payload + above + below


def body(state, cut_mask, fraction, neighbourhood, tile_flags, centroid_offset):
    args = (state, cut_mask, fraction, neighbourhood, tile_flags, centroid_offset)
    iy, ix = lax.axis_index("ty"), lax.axis_index("tx")
    even_y, even_x = iy % 2 == 0, ix % 2 == 0
    s0, s1, p0, p1, own_rows, own_cols = pack(*args)
    h0 = paired(s0, "ty", "tx", 0)
    h1 = paired(s1, "ty", "tx", 1)
    inner_out = inner(*args)
    top = jnp.where(even_y, h1, h0) * (iy > 0).astype(jnp.float32)
    bottom = jnp.where(even_y, h0, h1) * (iy < lax.axis_size("ty") - 1).astype(jnp.float32)
    c0 = paired(with_corners(p0, even_x, top, bottom), "tx", "ty", 0)
    c1 = paired(with_corners(p1, ~even_x, top, bottom), "tx", "ty", 1)
    return rim(h0, h1, c0, c1, own_rows, own_cols, inner_out)


def solution(mesh):
    placed = (
        P(None, "ty", "tx"),
        P("ty", "tx"),
        P("ty", "tx"),
        P("ty", "tx"),
        P("ty", "tx"),
        P(None, "ty", "tx"),
    )
    return jax.shard_map(
        body, mesh=mesh, in_specs=placed, out_specs=P(None, "ty", "tx"), check_vma=False
    )
```

```python
import functools

import jax
import jax.numpy as jnp
from jax import lax
from jax.experimental import pallas as pl
from jax.experimental.pallas import tpu as pltpu
from jax.sharding import PartitionSpec as P

DEPTH = 4
LANES = 128
FIELDS = 7
PACKED = 4 * FIELDS
MIB = 1024 * 1024
SPLIT = 7

courant = 0.1


def paired(value, axis, other, first):
    length, width = lax.axis_size(axis), lax.axis_size(other)
    pairs = []
    for i in range(length):
        for j in range(width):
            mate = (i + 1 if (i - first) % 2 == 0 else i - 1, j)
            if not 0 <= mate[0] < length:
                mate = (i, j ^ 1)
            here = i * width + j
            there = mate[0] * width + mate[1]
            pairs.append((here, there))
    if axis == "tx":
        swap = lambda k: (k % width) * length + k // width
        pairs = [(swap(a), swap(b)) for a, b in pairs]
    return lax.ppermute(value, ("ty", "tx"), sorted(pairs))


def lane_index():
    return lax.broadcasted_iota(jnp.int32, (8, LANES), 1)


def from_west(values, west, lane):
    return [
        pltpu.roll(jnp.where(lane == LANES - 1, values[west[t]], values[t]), 1, 1)
        for t in range(len(values))
    ]


def from_east(values, east, lane):
    return [
        pltpu.roll(jnp.where(lane == 0, values[east[t]], values[t]), LANES - 1, 1)
        for t in range(len(values))
    ]


def inverse(value):
    guess = pl.reciprocal(value, approx=True)
    return guess * (2.0 - value * guess)


def store_members(mk, code, kappa, t, rows, order):
    for b in range(9):
        held = (code & (1 << order[b])) != 0
        mk[b, t, rows, :] = jnp.where(held, kappa, 0.0)


plain_order = (0, 1, 2, 3, 4, 5, 6, 7, 8)
swapped_order = (0, 3, 6, 1, 4, 7, 2, 5, 8)


class Fields:
    def __init__(self, mk, raw, rc, seen, gath, cent, horiz, push):
        self.mk, self.raw, self.rc, self.seen = mk, raw, rc, seen
        self.gath, self.cent, self.horiz, self.push = gath, cent, horiz, push

    @staticmethod
    def shapes(tiles, rows):
        shape = lambda n: pltpu.VMEM((n, tiles, rows, LANES), jnp.float32)
        return [shape(9), shape(6), shape(1), shape(4), shape(18), shape(5), shape(14), shape(9)]


def at(ref, i, t, base, step=0):
    return ref[i, t, pl.ds(base + step, 8), :]


def stage_share(s, tiles, west, east, base):
    lane = lane_index()
    n = len(tiles)
    sums = []
    for dx in (-1, 0, 1):
        group = []
        for t in tiles:
            total = at(s.mk, 4 + dx, t, base)
            total = total + at(s.mk, 1 + dx, t, base, 1)
            total = total + at(s.mk, 7 + dx, t, base, -1)
            group.append(total)
        sums.append(group)
    low = from_east(sums[0], east, lane)
    high = from_west(sums[2], west, lane)
    centre = [[at(s.raw, 3 + f, t, base) for t in tiles] for f in range(3)]
    easts = [from_east(c, east, lane) for c in centre]
    wests = [from_west(c, west, lane) for c in centre]
    for i, move, step in ((0, from_west, -1.0), (1, from_east, 1.0)):
        beside = west if i == 0 else east
        x = move([at(s.raw, 1, t, base) for t in tiles], beside, lane)
        y = move([at(s.raw, 2, t, base) for t in tiles], beside, lane)
        for k, t in enumerate(tiles):
            s.seen[i, t, pl.ds(base, 8), :] = x[k] + step
            s.seen[2 + i, t, pl.ds(base, 8), :] = y[k]
    outs = [[] for _ in range(6)]
    for k, t in enumerate(tiles):
        coverage = jnp.maximum(sums[1][k] + low[k] + high[k], 0.125)
        rc = inverse(coverage)
        s.rc[0, t, pl.ds(base, 8), :] = rc
        share = at(s.raw, 0, t, base) * rc
        rate = (0.5 * courant) * rc
        keep = share - 4.0 * rate
        c = [centre[f][k] for f in range(3)]
        e = [easts[f][k] for f in range(3)]
        w = [wests[f][k] for f in range(3)]
        north = [at(s.raw, 3 + f, t, base, 1) for f in range(3)]
        south = [at(s.raw, 3 + f, t, base, -1) for f in range(3)]
        flux = [(e[1] - w[1]) + (north[2] - south[2]), e[0] - w[0], north[0] - south[0]]
        outs[0].append(share)
        outs[1].append(share * at(s.raw, 1, t, base))
        outs[2].append(share * at(s.raw, 2, t, base))
        for f in range(3):
            around = (e[f] + w[f]) + (north[f] + south[f])
            outs[3 + f].append(keep * c[f] - rate * (flux[f] - around))
    for f in range(6):
        w = from_west(outs[f], west, lane)
        e = from_east(outs[f], east, lane)
        for k, t in enumerate(tiles):
            s.gath[3 * f, t, pl.ds(base, 8), :] = w[k]
            s.gath[3 * f + 1, t, pl.ds(base, 8), :] = outs[f][k]
            s.gath[3 * f + 2, t, pl.ds(base, 8), :] = e[k]


def stage_average(s, tiles, base):
    for t in tiles:
        weight = {}
        for dy in (-1, 0, 1):
            for dx in (-1, 0, 1):
                member = at(s.mk, 3 * (dy + 1) + dx + 1, t, base)
                weight[dy, dx] = (member, member * at(s.gath, 1 + dx, t, base, dy))
        cols = [weight[-1, d][1] + weight[0, d][1] + weight[1, d][1] for d in (-1, 0, 1)]
        total = cols[0] + cols[1] + cols[2]
        upper = weight[1, -1][1] + weight[1, 0][1] + weight[1, 1][1]
        lower = weight[-1, -1][1] + weight[-1, 0][1] + weight[-1, 1][1]
        sums = [cols[2] - cols[0], upper - lower, None, None, None]
        for f in range(5):
            for dy in (-1, 0, 1):
                for dx in (-1, 0, 1):
                    term = weight[dy, dx][0] * at(s.gath, 3 * (f + 1) + 1 + dx, t, base, dy)
                    sums[f] = term if sums[f] is None else sums[f] + term
        inv = inverse(jnp.maximum(total, 1e-3))
        for f in range(5):
            s.cent[f, t, pl.ds(base, 8), :] = sums[f] * inv


def stage_horizontal(s, tiles, west, east, base):
    lane = lane_index()
    results = [[at(s.cent, f, t, base) for t in tiles] for f in range(5)]
    w = [from_west(r, west, lane) for r in results]
    e = [from_east(r, east, lane) for r in results]
    for k, t in enumerate(tiles):
        x = [w[0][k] - 1.0, results[0][k], e[0][k] + 1.0]
        v = [w[1][k], results[1][k], e[1][k]]
        a = [[w[2 + f][k], results[2 + f][k], e[2 + f][k]] for f in range(3)]
        add3 = lambda p: p[0] + p[1] + p[2]
        dot3 = lambda p, q: p[0] * q[0] + p[1] * q[1] + p[2] * q[2]
        made = [add3(x), add3(v), dot3(x, x), dot3(x, v), dot3(v, v)]
        made += [add3(a[f]) for f in range(3)]
        made += [dot3(x, a[f]) for f in range(3)]
        made += [dot3(v, a[f]) for f in range(3)]
        for i, value in enumerate(made):
            s.horiz[i, t, pl.ds(base, 8), :] = value


def stage_slope(s, tiles, base):
    for t in tiles:
        rows = lambda i: [at(s.horiz, i, t, base, d) for d in (-1, 0, 1)]
        add3 = lambda p: p[0] + p[1] + p[2]
        u, v = at(s.cent, 0, t, base), at(s.cent, 1, t, base)
        hx, hv = rows(0), rows(1)
        sum_x, sum_y = add3(hx), add3(hv)
        sum_xx = add3(rows(2)) + 1.0
        sum_xy = add3(rows(3)) + (hx[2] - hx[0])
        sum_yy = add3(rows(4)) + (2.0 * (hv[2] - hv[0]) + 7.0)
        mean_x = sum_x - 9.0 * u
        mean_y = sum_y - 9.0 * v
        moment_xx = sum_xx - u * (sum_x + mean_x)
        moment_yy = sum_yy - v * (sum_y + mean_y)
        moment_xy = sum_xy - u * sum_y - v * mean_x
        inv = inverse(moment_xx * moment_yy - moment_xy * moment_xy)
        moment_xx = moment_xx * inv
        moment_yy = moment_yy * inv
        moment_xy = moment_xy * inv
        for f in range(3):
            average = at(s.cent, 2 + f, t, base)
            ha = rows(5 + f)
            sum_a = add3(ha)
            right_x = add3(rows(8 + f)) - u * sum_a - average * mean_x
            right_y = add3(rows(11 + f)) + (ha[2] - ha[0]) - v * sum_a - average * mean_y
            slope_x = moment_yy * right_x - moment_xy * right_y
            slope_y = moment_xx * right_y - moment_xy * right_x
            s.push[f, t, pl.ds(base, 8), :] = average - slope_x * u - slope_y * v
            s.push[3 + f, t, pl.ds(base, 8), :] = slope_x
            s.push[6 + f, t, pl.ds(base, 8), :] = slope_y


def stage_push(s, tiles, west, east, base):
    lane = lane_index()
    groups = [[[] for _ in range(3)] for _ in range(3)]
    for t in tiles:
        for dx in (-1, 0, 1):
            if dx:
                x, middle = at(s.seen, (dx + 1) // 2, t, base), at(s.seen, 2 + (dx + 1) // 2, t, base)
            else:
                x, middle = at(s.raw, 1, t, base), at(s.raw, 2, t, base)
            totals = [None] * 3
            for dy in (-1, 0, 1):
                y = middle + float(dy) if dy else middle
                member = at(s.mk, 3 * (dy + 1) + dx + 1, t, base, -dy)
                for f in range(3):
                    plane = at(s.push, f, t, base, -dy)
                    plane = plane + at(s.push, 3 + f, t, base, -dy) * x
                    plane = plane + at(s.push, 6 + f, t, base, -dy) * y
                    term = member * plane
                    totals[f] = term if totals[f] is None else totals[f] + term
            for f in range(3):
                groups[dx + 1][f].append(totals[f])
    results = []
    for f in range(3):
        low = from_east(groups[0][f], east, lane)
        high = from_west(groups[2][f], west, lane)
        results.append(
            [
                (groups[1][f][k] + low[k] + high[k]) * at(s.rc, 0, t, base)
                for k, t in enumerate(tiles)
            ]
        )
    return results


def start_all(copies):
    for copy in copies:
        copy.start()
    for copy in copies:
        copy.wait()


def pack_kernel(
    state_in, cut_in, fraction_in, code_in, flags, offset_in,
    s0, s1, p0, p1, own_rows, own_cols, state, cut, fraction, code, offset, mix, sem,
):
    rows, cols = cut.shape
    bands = []
    for i, rs in enumerate((pl.ds(0, 8), pl.ds(rows - 8, 8), pl.ds(8, rows - 16))):
        pairs = [
            (cut_in.at[rs], cut.at[rs]),
            (code_in.at[rs], code.at[rs]),
            (fraction_in.at[rs], fraction.at[rs]),
            (offset_in.at[:, rs], offset.at[:, rs]),
            (state_in.at[:, rs], state.at[:, rs]),
        ]
        bands.append([pltpu.make_async_copy(a, b, sem.at[i, j]) for j, (a, b) in enumerate(pairs)])
    for band in bands:
        for copy in band:
            copy.start()
    for band in bands[:2]:
        for copy in band:
            copy.wait()
    ntile = cols // LANES
    even_y = lax.rem(lax.axis_index("ty"), 2) == 0
    even_x = lax.rem(lax.axis_index("tx"), 2) == 0

    def fields(rs, ls, flag):
        active = cut[rs, ls] > (1 - flag)
        return [
            jnp.where(active, code[rs, ls], 16).astype(jnp.float32),
            jnp.where(active, fraction[rs, ls].astype(jnp.float32) * (1.0 / 1024.0), 1.0),
            jnp.where(active, offset[0, rs, ls], 0.0),
            jnp.where(active, offset[1, rs, ls], 0.0),
            state[0, rs, ls],
            state[1, rs, ls],
            state[2, rs, ls],
        ]

    mids = {}
    for t in range(ntile):
        ls = pl.ds(t * LANES, LANES)
        made = []
        for i in range(2):
            got = fields(pl.ds(i * (rows - 8), 8), ls, flags[0, t])
            for f in range(FIELDS):
                own_rows[i, f, :, ls] = got[f]
            made.append(got)
        for f in range(FIELDS):
            top = made[0][f][0:4]
            bottom = made[1][f][4:8]
            s0[pl.ds(4 * f, 4), ls] = jnp.where(even_y, bottom, top)
            s1[pl.ds(4 * f, 4), ls] = jnp.where(even_y, top, bottom)
        if t in (0, ntile - 1):
            side = 0 if t == 0 else 1
            mids[side] = made
    for copy in bands[2]:
        copy.wait()
    for side, t in enumerate((0, ntile - 1)):
        got = fields(slice(None), pl.ds(t * LANES, LANES), flags[0, t])
        first = 0 if side == 0 else LANES - 8
        for f in range(FIELDS):
            own_cols[side, f, :, :] = got[f].T[first : first + 8, :]
    for f in range(FIELDS):
        left = own_cols[0, f, 0:4, :]
        right = own_cols[1, f, 4:8, :]
        rs = pl.ds(4 * f, 4)
        p0[rs, 0:LANES] = jnp.where(even_x, right, left)
        p1[rs, 0:LANES] = jnp.where(even_x, left, right)
        for side in range(2):
            first = 0 if side == 0 else LANES - 4
            near, far = mids[side][0][f], mids[side][1][f]
            for g, piece in ((1, near[0:4]), (2, near[4:8]), (3, far[0:4]), (4, far[4:8])):
                mix[side, g, rs, :] = pltpu.roll(piece, (4 * g - first) % LANES, 1)
    lane = lax.broadcasted_iota(jnp.int32, (PACKED, LANES), 1)
    parts = []
    for side in range(2):
        total = jnp.zeros((PACKED, LANES), jnp.float32)
        for g in range(1, 5):
            here = (lane >= 4 * g) & (lane < 4 * g + 4)
            total = jnp.where(here, mix[side, g, 0:PACKED, :], total)
        parts.append(total)
    p0[:, LANES:] = jnp.where(even_x, parts[1], parts[0])
    p1[:, LANES:] = jnp.where(even_x, parts[0], parts[1])


def in_vmem(value):
    return pltpu.with_memory_space_constraint(value, pltpu.VMEM)


VMEM_SPEC = pl.BlockSpec(memory_space=pltpu.VMEM)
SMEM_SPEC = pl.BlockSpec(memory_space=pltpu.SMEM)


def pack(state, cut, fraction, code, flags, offset):
    rows, cols = cut.shape
    strip = lambda *s: pltpu.VMEM(s, jnp.float32)
    ints = pltpu.VMEM((rows, cols), jnp.int32)
    hbm = pl.BlockSpec(memory_space=pltpu.HBM)
    held = lambda a: pltpu.with_memory_space_constraint(a, pltpu.HBM)
    made = pl.pallas_call(
        pack_kernel,
        out_shape=(
            strip(PACKED, cols), strip(PACKED, cols), strip(PACKED, 2 * LANES), strip(PACKED, 2 * LANES),
            strip(2, FIELDS, 8, cols), strip(2, FIELDS, 8, rows),
            strip(3, rows, cols), ints, ints, ints, strip(2, rows, cols),
        ),
        in_specs=[hbm] * 4 + [SMEM_SPEC, hbm],
        out_specs=[VMEM_SPEC] * 11,
        scratch_shapes=[pltpu.VMEM((2, 5, 32, LANES), jnp.float32), pltpu.SemaphoreType.DMA((3, 5))],
        compiler_params=pltpu.CompilerParams(vmem_limit_bytes=4 * MIB),
        name="pack",
    )(held(state), held(cut), held(fraction), held(code), flags, held(offset))
    return [in_vmem(m) for m in made]


def inner_kernel(first, last, state, cut, fraction, code, flags, offset, out, *rest):
    s = Fields(*rest[:8])
    rows, cols = cut.shape
    ntile = cols // LANES
    tiles = list(range(ntile))
    west = [(t - 1) % ntile for t in tiles]
    east = [(t + 1) % ntile for t in tiles]
    low, high = max(first - 1, 0), min(last + 1, rows // 8)

    def prepare(k, carry):
        src = pl.ds(pl.multiple_of(8 * (k + low), 8), 8)
        dst = pl.ds(pl.multiple_of(8 * k + 8, 8), 8)
        for t in tiles:
            ls = pl.ds(t * LANES, LANES)
            active = cut[src, ls] > (1 - flags[0, t])
            codes = jnp.where(active, code[src, ls], 16)
            kappa = jnp.where(active, fraction[src, ls].astype(jnp.float32) * (1.0 / 1024.0), 1.0)
            s.raw[0, t, dst, :] = kappa
            for i in range(2):
                s.raw[1 + i, t, dst, :] = jnp.where(active, offset[i, src, ls], 0.0)
            for f in range(3):
                s.raw[3 + f, t, dst, :] = state[f, src, ls]
            store_members(s.mk, codes, kappa, t, dst, plain_order)
        return carry

    def share(k, carry):
        for j in range(2):
            stage_share(s, tiles, west, east, 16 * k + 8 * j + 8)
        return carry

    def average(k, carry):
        stage_average(s, tiles, 8 * k + 8)
        return carry

    def horizontal(k, carry):
        stage_horizontal(s, tiles, west, east, 8 * k + 8)
        return carry

    def slope(k, carry):
        stage_slope(s, tiles, 8 * k + 8)
        return carry

    def push(k, carry):
        made = stage_push(s, tiles, west, east, 8 * (k + first - low) + 8)
        for f in range(3):
            for t in tiles:
                out[f, pl.ds(pl.multiple_of(8 * k, 8), 8), pl.ds(t * LANES, LANES)] = made[f][t]
        return carry

    count = high - low
    lax.fori_loop(0, count, prepare, 0)
    lax.fori_loop(0, (count + 1) // 2, share, 0)
    for step in (average, horizontal, slope):
        lax.fori_loop(0, count, step, 0)
    lax.fori_loop(0, last - first, push, 0)


def inner(first, last, state, cut, fraction, code, flags, offset):
    rows, cols = cut.shape
    ntile = cols // LANES
    count = last - first
    return pl.pallas_call(
        functools.partial(inner_kernel, first, last),
        out_shape=pltpu.VMEM((3, 8 * count, cols), jnp.float32),
        in_specs=[VMEM_SPEC] * 4 + [SMEM_SPEC, VMEM_SPEC],
        out_specs=VMEM_SPEC,
        scratch_shapes=Fields.shapes(ntile, 8 * count + 40),
        cost_estimate=pl.CostEstimate(
            flops=count * 4_000_000, transcendentals=0, bytes_accessed=count * 150_000
        ),
        compiler_params=pltpu.CompilerParams(vmem_limit_bytes=28 * MIB),
        name=f"inner{first}",
    )(state, cut, fraction, code, flags, offset)


swap_fields = (0, 1, 3, 2, 4, 6, 5)


def rim_kernel(h0, h1, c0, c1, own_rows, own_cols, base_ref, low_part, high_part, out, wide, *rest):
    s = Fields(*rest[:8])
    res, turn, edge_c, edge_r, sem = rest[8:]
    _, rows, cols = out.shape
    ntile = cols // LANES
    split = low_part.shape[1]
    middle = pl.ds(LANES, cols - 2 * LANES)
    early = [
        pltpu.make_async_copy(
            low_part.at[:, pl.ds(8, split - 8), middle], out.at[:, pl.ds(8, split - 8), middle], sem.at[2, 0]
        ),
        pltpu.make_async_copy(
            high_part.at[:, pl.ds(0, rows - split - 8), middle],
            out.at[:, pl.ds(split, rows - split - 8), middle],
            sem.at[2, 1],
        ),
    ]
    for copy in early:
        copy.start()
    iy, ix = lax.axis_index("ty"), lax.axis_index("tx")
    even_y, even_x = lax.rem(iy, 2) == 0, lax.rem(ix, 2) == 0
    have_top, have_bottom = iy > 0, iy < lax.axis_size("ty") - 1
    have_left, have_right = ix > 0, ix < lax.axis_size("tx") - 1
    group = ntile + 1
    top, bottom, left, right = 0, group, 2 * group, 2 * group + 1
    zero4 = jnp.zeros((4, LANES), jnp.float32)
    halo = lambda even, a, b, have: jnp.where(have, jnp.where(even, a, b), zero4)
    for f in range(FIELDS):
        rs = pl.ds(4 * f, 4)
        for t in range(ntile):
            ls = pl.ds(t * LANES, LANES)
            wide[f, top + t, 0:4, :] = halo(even_y, h1[rs, ls], h0[rs, ls], have_top)
            wide[f, top + t, 4:12, :] = own_rows[0, f, :, ls]
            wide[f, bottom + t, 0:8, :] = own_rows[1, f, :, ls]
            wide[f, bottom + t, 8:12, :] = halo(even_y, h0[rs, ls], h1[rs, ls], have_bottom)
        fe = swap_fields[f]
        wide[fe, left, 0:4, :] = halo(even_x, c1[rs, 0:LANES], c0[rs, 0:LANES], have_left)
        wide[fe, left, 4:12, :] = own_cols[0, f, :, :]
        wide[fe, right, 0:8, :] = own_cols[1, f, :, :]
        wide[fe, right, 8:12, :] = halo(even_x, c0[rs, 0:LANES], c1[rs, 0:LANES], have_right)
    lane = lax.broadcasted_iota(jnp.int32, (PACKED, LANES), 1)
    none = jnp.zeros((PACKED, LANES), jnp.float32)
    a, b = c0[:, LANES:], c1[:, LANES:]
    from_left = jnp.where(have_left, jnp.where(even_x, b, a), none)
    from_right = jnp.where(have_right, jnp.where(even_x, a, b), none)
    for g in range(6):
        l = pltpu.roll(from_left, LANES - 4 - 4 * g, 1)
        r = pltpu.roll(from_right, (LANES - 4 * g) % LANES, 1)
        both = jnp.where(lane < 4, r, jnp.where(lane >= LANES - 4, l, 0.0))
        strip, first = ((top, 4 * g) if g < 3 else (bottom, 4 * (g - 3)))
        for f in range(FIELDS):
            wide[f, strip + ntile, first : first + 4, :] = both[4 * f : 4 * f + 4, :]

    tiles = list(range(2 * group + 2))
    west, east = list(tiles), list(tiles)
    for first in (top, bottom):
        for t in range(group):
            west[first + t] = first + (t - 1) % group
            east[first + t] = first + (t + 1) % group
    base = base_ref[0]
    for t in tiles:
        order = plain_order if t < left else swapped_order
        for r in range(2):
            rs = pl.ds(8 * r, 8)
            kappa = wide[1, t, rs, :]
            store_members(s.mk, wide[0, t, rs, :].astype(jnp.int32), kappa, t, rs, order)
            s.raw[0, t, rs, :] = kappa
            for f in range(2, FIELDS):
                s.raw[f - 1, t, rs, :] = wide[f, t, rs, :]
    for first in (0, 5, 10):
        pick = tiles[first : first + 5]
        w = [west[t] - first for t in pick]
        e = [east[t] - first for t in pick]
        stage_share(s, pick, w, e, base + 1)
        stage_share(s, pick, w, e, base + 9)
        stage_average(s, pick, base + 2)
        stage_horizontal(s, pick, w, e, base + 2)
        stage_slope(s, pick, base + 3)
        made = stage_push(s, pick, w, e, base + 4)
        for f in range(3):
            for k, t in enumerate(pick):
                res[f, t, :, :] = made[f][k]
    turn[...] = jnp.zeros_like(turn)
    for f in range(3):
        fe = (0, 2, 1)[f]
        turn[pl.ds(4 * f, 4), :] = res[fe, left, 0:4, :]
        turn[pl.ds(16 + 4 * f, 4), :] = res[fe, right, 0:4, :]
    back = turn[...].T
    lane = lax.broadcasted_iota(jnp.int32, (rows, LANES), 1)
    for f in range(3):
        left_cols = pltpu.roll(back, (LANES - 4 * f) % LANES, 1)
        right_cols = pltpu.roll(back, LANES - 4 - 16 - 4 * f, 1)
        for part, rs in ((low_part, slice(0, split)), (high_part, slice(split, rows))):
            edge_c[0, f, rs] = jnp.where(lane[rs] < 4, left_cols[rs], part[f, :, 0:LANES])
            edge_c[1, f, rs] = jnp.where(
                lane[rs] >= LANES - 4, right_cols[rs], part[f, :, cols - LANES :]
            )
        edge_r[0, f] = low_part[f, 0:8, LANES : cols - LANES]
        edge_r[1, f] = high_part[f, rows - split - 8 :, LANES : cols - LANES]
        for i, t in enumerate((0, ntile - 1)):
            edge_c[i, f, 0:4, :] = res[f, top + t, 0:4, :]
            edge_c[i, f, rows - 4 : rows, :] = res[f, bottom + t, 0:4, :]
        for t in range(1, ntile - 1):
            ls = pl.ds((t - 1) * LANES, LANES)
            edge_r[0, f, 0:4, ls] = res[f, top + t, 0:4, :]
            edge_r[1, f, 4:8, ls] = res[f, bottom + t, 0:4, :]
    writes = []
    for i, col in enumerate((0, cols - LANES)):
        writes.append(
            pltpu.make_async_copy(edge_c.at[i], out.at[:, :, pl.ds(col, LANES)], sem.at[0, i])
        )
    for i, row in enumerate((0, rows - 8)):
        writes.append(
            pltpu.make_async_copy(
                edge_r.at[i], out.at[:, pl.ds(row, 8), pl.ds(LANES, cols - 2 * LANES)], sem.at[1, i]
            )
        )
    start_all(writes)
    for copy in early:
        copy.wait()


def rim(h0, h1, c0, c1, own_rows, own_cols, low_part, high_part):
    cols = low_part.shape[2]
    rows = low_part.shape[1] + high_part.shape[1]
    ntile = cols // LANES
    tiles = 2 * (ntile + 1) + 2
    f32 = jnp.float32
    return pl.pallas_call(
        rim_kernel,
        out_shape=jax.ShapeDtypeStruct((3, rows, cols), f32),
        in_specs=[VMEM_SPEC] * 6 + [SMEM_SPEC] + [VMEM_SPEC] * 2,
        out_specs=pl.BlockSpec(memory_space=pl.ANY),
        scratch_shapes=[pltpu.VMEM((FIELDS, tiles, 16, LANES), f32)]
        + Fields.shapes(tiles, 24)
        + [
            pltpu.VMEM((3, tiles, 8, LANES), f32),
            pltpu.VMEM((LANES, LANES), f32),
            pltpu.VMEM((2, 3, rows, LANES), f32),
            pltpu.VMEM((2, 3, 8, cols - 2 * LANES), f32),
            pltpu.SemaphoreType.DMA((3, 2)),
        ],
        cost_estimate=pl.CostEstimate(flops=10_000_000, transcendentals=0, bytes_accessed=1_000_000),
        compiler_params=pltpu.CompilerParams(vmem_limit_bytes=24 * MIB),
        name="rim",
    )(h0, h1, c0, c1, own_rows, own_cols, jnp.zeros((1,), jnp.int32), low_part, high_part)


def corner_kernel(h0, h1, p0, p1, after, q0, q1):
    iy, ix = lax.axis_index("ty"), lax.axis_index("tx")
    even_y, even_x = lax.rem(iy, 2) == 0, lax.rem(ix, 2) == 0
    have_top, have_bottom = iy > 0, iy < lax.axis_size("ty") - 1
    cols = h0.shape[1]
    lane = lax.broadcasted_iota(jnp.int32, (PACKED, LANES), 1)
    corners = []
    for first, ls in ((0, pl.ds(0, LANES)), (LANES - 4, pl.ds(cols - LANES, LANES))):
        a, b = h0[:, ls], h1[:, ls]
        above = jnp.where(have_top, jnp.where(even_y, b, a), 0.0)
        below = jnp.where(have_bottom, jnp.where(even_y, a, b), 0.0)
        above = pltpu.roll(above, (LANES - first) % LANES, 1)
        below = pltpu.roll(below, (20 + LANES - first) % LANES, 1)
        total = jnp.where(lane < 4, above, 0.0)
        corners.append(jnp.where((lane >= 20) & (lane < 24), below, total))
    left, right = corners
    q0[:, 0:LANES] = p0[:, 0:LANES]
    q1[:, 0:LANES] = p1[:, 0:LANES]
    q0[:, LANES:] = p0[:, LANES:] + jnp.where(even_x, right, left)
    q1[:, LANES:] = p1[:, LANES:] + jnp.where(even_x, left, right)


def with_corners(h0, h1, p0, p1, after):
    return pl.pallas_call(
        corner_kernel,
        out_shape=(pltpu.VMEM(p0.shape, jnp.float32), pltpu.VMEM(p1.shape, jnp.float32)),
        in_specs=[VMEM_SPEC] * 5,
        out_specs=[VMEM_SPEC] * 2,
        compiler_params=pltpu.CompilerParams(vmem_limit_bytes=2 * MIB),
        name="corner",
    )(h0, h1, p0, p1, after)


def body(state, cut_mask, fraction, neighbourhood, tile_flags, centroid_offset):
    s0, s1, p0, p1, own_rows, own_cols, *held = pack(
        state, cut_mask, fraction, neighbourhood, tile_flags, centroid_offset
    )
    args = (*held[:4], tile_flags, held[4])
    h0 = in_vmem(paired(s0, "ty", "tx", 0))
    h1 = in_vmem(paired(s1, "ty", "tx", 1))
    low_part = in_vmem(inner(0, SPLIT, *args))
    q0, q1 = with_corners(h0, h1, p0, p1, low_part)
    c0 = in_vmem(paired(q0, "tx", "ty", 0))
    c1 = in_vmem(paired(q1, "tx", "ty", 1))
    high_part = in_vmem(inner(SPLIT, state.shape[1] // 8, *args))
    return rim(h0, h1, c0, c1, own_rows, own_cols, low_part, high_part)


def solution(mesh):
    placed = (
        P(None, "ty", "tx"),
        P("ty", "tx"),
        P("ty", "tx"),
        P("ty", "tx"),
        P("ty", "tx"),
        P(None, "ty", "tx"),
    )
    return jax.shard_map(
        body, mesh=mesh, in_specs=placed, out_specs=P(None, "ty", "tx"), check_vma=False
    )
```

```python
import functools

import jax
import jax.numpy as jnp
from jax import lax
from jax.experimental import pallas as pl
from jax.experimental.pallas import tpu as pltpu
from jax.sharding import PartitionSpec as P

DEPTH = 4
LANES = 128
FIELDS = 7
PACKED = 4 * FIELDS
MIB = 1024 * 1024
ORIGIN = 8

courant = 0.1


def paired(value, axis, other, first):
    length, width = lax.axis_size(axis), lax.axis_size(other)
    pairs = []
    for i in range(length):
        for j in range(width):
            mate = (i + 1 if (i - first) % 2 == 0 else i - 1, j)
            if not 0 <= mate[0] < length:
                mate = (i, j ^ 1)
            here = i * width + j
            there = mate[0] * width + mate[1]
            pairs.append((here, there))
    if axis == "tx":
        swap = lambda k: (k % width) * length + k // width
        pairs = [(swap(a), swap(b)) for a, b in pairs]
    return lax.ppermute(value, ("ty", "tx"), sorted(pairs))


def lane_index():
    return lax.broadcasted_iota(jnp.int32, (8, LANES), 1)


def from_west(values, west, lane):
    return [
        pltpu.roll(jnp.where(lane == LANES - 1, values[west[t]], values[t]), 1, 1)
        for t in range(len(values))
    ]


def from_east(values, east, lane):
    return [
        pltpu.roll(jnp.where(lane == 0, values[east[t]], values[t]), LANES - 1, 1)
        for t in range(len(values))
    ]


def inverse(value):
    guess = pl.reciprocal(value, approx=True)
    return guess * (2.0 - value * guess)


def store_members(mk, code, kappa, t, rows, order):
    for b in range(9):
        held = (code & (1 << order[b])) != 0
        mk[b, t, rows, :] = jnp.where(held, kappa, 0.0)


plain_order = (0, 1, 2, 3, 4, 5, 6, 7, 8)
swapped_order = (0, 3, 6, 1, 4, 7, 2, 5, 8)


class Fields:
    def __init__(self, mk, raw, rc, seen, gath, cent, horiz, push):
        self.mk, self.raw, self.rc, self.seen = mk, raw, rc, seen
        self.gath, self.cent, self.horiz, self.push = gath, cent, horiz, push

    @staticmethod
    def shapes(tiles, rows):
        shape = lambda n: pltpu.VMEM((n, tiles, rows, LANES), jnp.float32)
        return [shape(9), shape(6), shape(1), shape(4), shape(18), shape(5), shape(14), shape(9)]


def at(ref, i, t, base, step=0):
    return ref[i, t, pl.ds(base + step, 8), :]


def stage_share(s, tiles, west, east, base):
    lane = lane_index()
    n = len(tiles)
    sums = []
    for dx in (-1, 0, 1):
        group = []
        for t in tiles:
            total = at(s.mk, 4 + dx, t, base)
            total = total + at(s.mk, 1 + dx, t, base, 1)
            total = total + at(s.mk, 7 + dx, t, base, -1)
            group.append(total)
        sums.append(group)
    low = from_east(sums[0], east, lane)
    high = from_west(sums[2], west, lane)
    centre = [[at(s.raw, 3 + f, t, base) for t in tiles] for f in range(3)]
    easts = [from_east(c, east, lane) for c in centre]
    wests = [from_west(c, west, lane) for c in centre]
    for i, move, step in ((0, from_west, -1.0), (1, from_east, 1.0)):
        beside = west if i == 0 else east
        x = move([at(s.raw, 1, t, base) for t in tiles], beside, lane)
        y = move([at(s.raw, 2, t, base) for t in tiles], beside, lane)
        for k, t in enumerate(tiles):
            s.seen[i, t, pl.ds(base, 8), :] = x[k] + step
            s.seen[2 + i, t, pl.ds(base, 8), :] = y[k]
    outs = [[] for _ in range(6)]
    for k, t in enumerate(tiles):
        coverage = jnp.maximum(sums[1][k] + low[k] + high[k], 0.125)
        rc = inverse(coverage)
        s.rc[0, t, pl.ds(base, 8), :] = rc
        share = at(s.raw, 0, t, base) * rc
        rate = (0.5 * courant) * rc
        keep = share - 4.0 * rate
        c = [centre[f][k] for f in range(3)]
        e = [easts[f][k] for f in range(3)]
        w = [wests[f][k] for f in range(3)]
        north = [at(s.raw, 3 + f, t, base, 1) for f in range(3)]
        south = [at(s.raw, 3 + f, t, base, -1) for f in range(3)]
        flux = [(e[1] - w[1]) + (north[2] - south[2]), e[0] - w[0], north[0] - south[0]]
        outs[0].append(share)
        outs[1].append(share * at(s.raw, 1, t, base))
        outs[2].append(share * at(s.raw, 2, t, base))
        for f in range(3):
            around = (e[f] + w[f]) + (north[f] + south[f])
            outs[3 + f].append(keep * c[f] - rate * (flux[f] - around))
    for f in range(6):
        w = from_west(outs[f], west, lane)
        e = from_east(outs[f], east, lane)
        for k, t in enumerate(tiles):
            s.gath[3 * f, t, pl.ds(base, 8), :] = w[k]
            s.gath[3 * f + 1, t, pl.ds(base, 8), :] = outs[f][k]
            s.gath[3 * f + 2, t, pl.ds(base, 8), :] = e[k]


def stage_average(s, tiles, base):
    for t in tiles:
        weight = {}
        for dy in (-1, 0, 1):
            for dx in (-1, 0, 1):
                member = at(s.mk, 3 * (dy + 1) + dx + 1, t, base)
                weight[dy, dx] = (member, member * at(s.gath, 1 + dx, t, base, dy))
        cols = [weight[-1, d][1] + weight[0, d][1] + weight[1, d][1] for d in (-1, 0, 1)]
        total = cols[0] + cols[1] + cols[2]
        upper = weight[1, -1][1] + weight[1, 0][1] + weight[1, 1][1]
        lower = weight[-1, -1][1] + weight[-1, 0][1] + weight[-1, 1][1]
        sums = [cols[2] - cols[0], upper - lower, None, None, None]
        for f in range(5):
            for dy in (-1, 0, 1):
                for dx in (-1, 0, 1):
                    term = weight[dy, dx][0] * at(s.gath, 3 * (f + 1) + 1 + dx, t, base, dy)
                    sums[f] = term if sums[f] is None else sums[f] + term
        inv = inverse(jnp.maximum(total, 1e-3))
        for f in range(5):
            s.cent[f, t, pl.ds(base, 8), :] = sums[f] * inv


def stage_horizontal(s, tiles, west, east, base):
    lane = lane_index()
    results = [[at(s.cent, f, t, base) for t in tiles] for f in range(5)]
    w = [from_west(r, west, lane) for r in results]
    e = [from_east(r, east, lane) for r in results]
    for k, t in enumerate(tiles):
        x = [w[0][k] - 1.0, results[0][k], e[0][k] + 1.0]
        v = [w[1][k], results[1][k], e[1][k]]
        a = [[w[2 + f][k], results[2 + f][k], e[2 + f][k]] for f in range(3)]
        add3 = lambda p: p[0] + p[1] + p[2]
        dot3 = lambda p, q: p[0] * q[0] + p[1] * q[1] + p[2] * q[2]
        made = [add3(x), add3(v), dot3(x, x), dot3(x, v), dot3(v, v)]
        made += [add3(a[f]) for f in range(3)]
        made += [dot3(x, a[f]) for f in range(3)]
        made += [dot3(v, a[f]) for f in range(3)]
        for i, value in enumerate(made):
            s.horiz[i, t, pl.ds(base, 8), :] = value


def stage_slope(s, tiles, base):
    for t in tiles:
        rows = lambda i: [at(s.horiz, i, t, base, d) for d in (-1, 0, 1)]
        add3 = lambda p: p[0] + p[1] + p[2]
        u, v = at(s.cent, 0, t, base), at(s.cent, 1, t, base)
        hx, hv = rows(0), rows(1)
        sum_x, sum_y = add3(hx), add3(hv)
        sum_xx = add3(rows(2)) + 1.0
        sum_xy = add3(rows(3)) + (hx[2] - hx[0])
        sum_yy = add3(rows(4)) + (2.0 * (hv[2] - hv[0]) + 7.0)
        mean_x = sum_x - 9.0 * u
        mean_y = sum_y - 9.0 * v
        moment_xx = sum_xx - u * (sum_x + mean_x)
        moment_yy = sum_yy - v * (sum_y + mean_y)
        moment_xy = sum_xy - u * sum_y - v * mean_x
        inv = inverse(moment_xx * moment_yy - moment_xy * moment_xy)
        moment_xx = moment_xx * inv
        moment_yy = moment_yy * inv
        moment_xy = moment_xy * inv
        for f in range(3):
            average = at(s.cent, 2 + f, t, base)
            ha = rows(5 + f)
            sum_a = add3(ha)
            right_x = add3(rows(8 + f)) - u * sum_a - average * mean_x
            right_y = add3(rows(11 + f)) + (ha[2] - ha[0]) - v * sum_a - average * mean_y
            slope_x = moment_yy * right_x - moment_xy * right_y
            slope_y = moment_xx * right_y - moment_xy * right_x
            s.push[f, t, pl.ds(base, 8), :] = average - slope_x * u - slope_y * v
            s.push[3 + f, t, pl.ds(base, 8), :] = slope_x
            s.push[6 + f, t, pl.ds(base, 8), :] = slope_y


def stage_push(s, tiles, west, east, base):
    lane = lane_index()
    groups = [[[] for _ in range(3)] for _ in range(3)]
    for t in tiles:
        for dx in (-1, 0, 1):
            if dx:
                x, middle = at(s.seen, (dx + 1) // 2, t, base), at(s.seen, 2 + (dx + 1) // 2, t, base)
            else:
                x, middle = at(s.raw, 1, t, base), at(s.raw, 2, t, base)
            totals = [None] * 3
            for dy in (-1, 0, 1):
                y = middle + float(dy) if dy else middle
                member = at(s.mk, 3 * (dy + 1) + dx + 1, t, base, -dy)
                for f in range(3):
                    plane = at(s.push, f, t, base, -dy)
                    plane = plane + at(s.push, 3 + f, t, base, -dy) * x
                    plane = plane + at(s.push, 6 + f, t, base, -dy) * y
                    term = member * plane
                    totals[f] = term if totals[f] is None else totals[f] + term
            for f in range(3):
                groups[dx + 1][f].append(totals[f])
    results = []
    for f in range(3):
        low = from_east(groups[0][f], east, lane)
        high = from_west(groups[2][f], west, lane)
        results.append(
            [
                (groups[1][f][k] + low[k] + high[k]) * at(s.rc, 0, t, base)
                for k, t in enumerate(tiles)
            ]
        )
    return results


def start_all(copies):
    for copy in copies:
        copy.start()
    for copy in copies:
        copy.wait()


def strip_fields(state, cut, fraction, code, offset, rs, ls, limit):
    active = cut[rs, ls] > limit
    return [
        jnp.where(active, code[rs, ls], 16).astype(jnp.float32),
        jnp.where(active, fraction[rs, ls].astype(jnp.float32) * (1.0 / 1024.0), 1.0),
        jnp.where(active, offset[0, rs, ls], 0.0),
        jnp.where(active, offset[1, rs, ls], 0.0),
        state[0, rs, ls],
        state[1, rs, ls],
        state[2, rs, ls],
    ]


def pack_kernel(
    state_in, cut_in, fraction_in, code_in, flags_in, offset_in,
    s0, s1, own_rows, limit, state, cut, fraction, code, offset, flags, sem,
):
    rows, cols = cut_in.shape
    copies = [pltpu.make_async_copy(flags_in, flags, sem.at[2, 0])]
    for i in range(2):
        rs, to = pl.ds(i * (rows - 8), 8), pl.ds(8 * i, 8)
        pairs = [
            (cut_in.at[rs], cut.at[to]),
            (code_in.at[rs], code.at[to]),
            (fraction_in.at[rs], fraction.at[to]),
            (offset_in.at[:, rs], offset.at[:, to]),
            (state_in.at[:, rs], state.at[:, to]),
        ]
        copies += [pltpu.make_async_copy(a, b, sem.at[i, j]) for j, (a, b) in enumerate(pairs)]
    start_all(copies)
    even_y = lax.rem(lax.axis_index("ty"), 2) == 0
    for t in range(cols // LANES):
        ls = pl.ds(t * LANES, LANES)
        level = 1 - flags[0, t]
        limit[:, ls] = jnp.full((8, LANES), level, jnp.int32)
        made = []
        for i in range(2):
            got = strip_fields(state, cut, fraction, code, offset, pl.ds(8 * i, 8), ls, level)
            for f in range(FIELDS):
                own_rows[i, f, :, ls] = got[f]
            made.append(got)
        for f in range(FIELDS):
            top = made[0][f][0:4]
            bottom = made[1][f][4:8]
            s0[pl.ds(4 * f, 4), ls] = jnp.where(even_y, bottom, top)
            s1[pl.ds(4 * f, 4), ls] = jnp.where(even_y, top, bottom)


def in_vmem(value):
    return pltpu.with_memory_space_constraint(value, pltpu.VMEM)


def in_hbm(value):
    return pltpu.with_memory_space_constraint(value, pltpu.HBM)


VMEM_SPEC = pl.BlockSpec(memory_space=pltpu.VMEM)
SMEM_SPEC = pl.BlockSpec(memory_space=pltpu.SMEM)
HBM_SPEC = pl.BlockSpec(memory_space=pltpu.HBM)


def pack(*args):
    cols = args[1].shape[1]
    f32, i32 = jnp.float32, jnp.int32
    made = pl.pallas_call(
        pack_kernel,
        out_shape=(
            pltpu.VMEM((PACKED, cols), f32), pltpu.VMEM((PACKED, cols), f32),
            pltpu.VMEM((2, FIELDS, 8, cols), f32), pltpu.VMEM((8, cols), i32),
        ),
        in_specs=[HBM_SPEC] * 6,
        out_specs=[VMEM_SPEC] * 4,
        scratch_shapes=[
            pltpu.VMEM((3, 16, cols), f32),
            pltpu.VMEM((16, cols), i32),
            pltpu.VMEM((16, cols), i32),
            pltpu.VMEM((16, cols), i32),
            pltpu.VMEM((2, 16, cols), f32),
            pltpu.SMEM((1, cols // LANES), i32),
            pltpu.SemaphoreType.DMA((3, 5)),
        ],
        compiler_params=pltpu.CompilerParams(vmem_limit_bytes=2 * MIB),
        name="pack",
    )(*[in_hbm(a) for a in args])
    return [in_vmem(m) for m in made]


def first_kernel(
    state, cut, fraction, code, offset, limit, own_rows, p0, p1, own_cols, mk, raw, rc, seen, cent, gath, mix
):
    s = Fields(mk, raw, rc, seen, gath, cent, None, None)
    rows, cols = cut.shape
    ntile = cols // LANES
    tiles = list(range(ntile))
    west = [(t - 1) % ntile for t in tiles]
    east = [(t + 1) % ntile for t in tiles]

    even_x = lax.rem(lax.axis_index("tx"), 2) == 0
    for side, t in enumerate((0, ntile - 1)):
        ls = pl.ds(t * LANES, LANES)
        got = strip_fields(state, cut, fraction, code, offset, slice(None), ls, limit[0:1, ls])
        first = 0 if side == 0 else LANES - 8
        for f in range(FIELDS):
            own_cols[side, f, :, :] = got[f].T[first : first + 8, :]
    for f in range(FIELDS):
        left = own_cols[0, f, 0:4, :]
        right = own_cols[1, f, 4:8, :]
        rs = pl.ds(4 * f, 4)
        p0[rs, 0:LANES] = jnp.where(even_x, right, left)
        p1[rs, 0:LANES] = jnp.where(even_x, left, right)
        for side in range(2):
            ls = pl.ds(side * (cols - LANES), LANES)
            first = 0 if side == 0 else LANES - 4
            near, far = own_rows[0, f, :, ls], own_rows[1, f, :, ls]
            for g, piece in ((1, near[0:4]), (2, near[4:8]), (3, far[0:4]), (4, far[4:8])):
                mix[side, g, rs, :] = pltpu.roll(piece, (4 * g - first) % LANES, 1)
    lane = lax.broadcasted_iota(jnp.int32, (PACKED, LANES), 1)
    parts = []
    for side in range(2):
        total = jnp.zeros((PACKED, LANES), jnp.float32)
        for g in range(1, 5):
            here = (lane >= 4 * g) & (lane < 4 * g + 4)
            total = jnp.where(here, mix[side, g, 0:PACKED, :], total)
        parts.append(total)
    p0[:, LANES:] = jnp.where(even_x, parts[1], parts[0])
    p1[:, LANES:] = jnp.where(even_x, parts[0], parts[1])

    def prepare(k, carry):
        src = pl.ds(pl.multiple_of(8 * k, 8), 8)
        dst = pl.ds(pl.multiple_of(8 * k + ORIGIN, 8), 8)
        for t in tiles:
            ls = pl.ds(t * LANES, LANES)
            active = cut[src, ls] > limit[:, ls]
            codes = jnp.where(active, code[src, ls], 16)
            kappa = jnp.where(active, fraction[src, ls].astype(jnp.float32) * (1.0 / 1024.0), 1.0)
            s.raw[0, t, dst, :] = kappa
            for i in range(2):
                s.raw[1 + i, t, dst, :] = jnp.where(active, offset[i, src, ls], 0.0)
            for f in range(3):
                s.raw[3 + f, t, dst, :] = state[f, src, ls]
            store_members(s.mk, codes, kappa, t, dst, plain_order)
        return carry

    def sweep(k, carry):
        stage_share(s, tiles, west, east, 8 * k + ORIGIN)
        return carry

    def sweep2(k, carry):
        stage_average(s, tiles, 8 * k + ORIGIN)
        return carry

    lax.fori_loop(0, rows // 8, prepare, 0)
    lax.fori_loop(0, rows // 8, sweep, 0)
    lax.fori_loop(0, rows // 8, sweep2, 0)


def second_kernel(mk, raw, rc, seen, cent, out, horiz, push):
    s = Fields(mk, raw, rc, seen, None, cent, horiz, push)
    ntile = mk.shape[1]
    count = out.shape[1] // 8
    tiles = list(range(ntile))
    west = [(t - 1) % ntile for t in tiles]
    east = [(t + 1) % ntile for t in tiles]

    def slopes(k, carry):
        stage_horizontal(s, tiles, west, east, 8 * k + ORIGIN)
        return carry

    def slopes2(k, carry):
        stage_slope(s, tiles, 8 * k + ORIGIN)
        return carry

    def spread(k, carry):
        made = stage_push(s, tiles, west, east, 8 * k + ORIGIN)
        for f in range(3):
            for t in tiles:
                out[f, pl.ds(pl.multiple_of(8 * k, 8), 8), pl.ds(t * LANES, LANES)] = made[f][t]
        return carry

    lax.fori_loop(0, count, slopes, 0)
    lax.fori_loop(0, count, slopes2, 0)
    lax.fori_loop(0, count, spread, 0)


def first_part(state, cut, fraction, code, offset, limit, own_rows):
    rows, cols = cut.shape
    ntile = cols // LANES
    f32 = jnp.float32
    mk, raw, rc, seen, gath, cent, _, _ = Fields.shapes(ntile, rows + 16)
    made = pl.pallas_call(
        first_kernel,
        out_shape=(
            pltpu.VMEM((PACKED, 2 * LANES), f32), pltpu.VMEM((PACKED, 2 * LANES), f32),
            pltpu.VMEM((2, FIELDS, 8, rows), f32), mk, raw, rc, seen, cent,
        ),
        in_specs=[VMEM_SPEC] * 7,
        out_specs=[VMEM_SPEC] * 8,
        scratch_shapes=[gath, pltpu.VMEM((2, 5, 32, LANES), f32)],
        compiler_params=pltpu.CompilerParams(vmem_limit_bytes=10 * MIB),
        cost_estimate=pl.CostEstimate(flops=30_000_000, transcendentals=0, bytes_accessed=1_000_000),
        name="first",
    )(state, cut, fraction, code, offset, limit, own_rows)
    return [in_vmem(m) for m in made]


def second_part(rows, *held):
    ntile = held[0].shape[1]
    *_, horiz, push = Fields.shapes(ntile, rows + 16)
    return in_vmem(
        pl.pallas_call(
            second_kernel,
            out_shape=pltpu.VMEM((3, rows, ntile * LANES), jnp.float32),
            in_specs=[VMEM_SPEC] * 5,
            out_specs=VMEM_SPEC,
            scratch_shapes=[horiz, push],
            compiler_params=pltpu.CompilerParams(vmem_limit_bytes=12 * MIB),
            cost_estimate=pl.CostEstimate(flops=30_000_000, transcendentals=0, bytes_accessed=1_000_000),
            name="second",
        )(*held)
    )


swap_fields = (0, 1, 3, 2, 4, 6, 5)


def rim_kernel(h0, h1, c0, c1, own_rows, own_cols, base_ref, inner_out, out, wide, *rest):
    s = Fields(*rest[:8])
    turn, edge_c, edge_r, sem = rest[8:]
    _, rows, cols = out.shape
    ntile = cols // LANES
    inside = pl.ds(8, rows - 16)
    middle = pl.ds(LANES, cols - 2 * LANES)
    writes = [pltpu.make_async_copy(inner_out.at[:, inside, middle], out.at[:, inside, middle], sem.at[0])]
    writes[0].start()
    iy, ix = lax.axis_index("ty"), lax.axis_index("tx")
    even_y, even_x = lax.rem(iy, 2) == 0, lax.rem(ix, 2) == 0
    have_top, have_bottom = iy > 0, iy < lax.axis_size("ty") - 1
    have_left, have_right = ix > 0, ix < lax.axis_size("tx") - 1
    group = ntile + 1
    top, bottom, left, right = 0, group, 2 * group, 2 * group + 1
    zero4 = jnp.zeros((4, LANES), jnp.float32)
    halo = lambda even, a, b, have: jnp.where(have, jnp.where(even, a, b), zero4)
    for f in range(FIELDS):
        rs = pl.ds(4 * f, 4)
        for t in range(ntile):
            ls = pl.ds(t * LANES, LANES)
            wide[f, top + t, 0:4, :] = halo(even_y, h1[rs, ls], h0[rs, ls], have_top)
            wide[f, top + t, 4:12, :] = own_rows[0, f, :, ls]
            wide[f, bottom + t, 0:8, :] = own_rows[1, f, :, ls]
            wide[f, bottom + t, 8:12, :] = halo(even_y, h0[rs, ls], h1[rs, ls], have_bottom)
        fe = swap_fields[f]
        wide[fe, left, 0:4, :] = halo(even_x, c1[rs, 0:LANES], c0[rs, 0:LANES], have_left)
        wide[fe, left, 4:12, :] = own_cols[0, f, :, :]
        wide[fe, right, 0:8, :] = own_cols[1, f, :, :]
        wide[fe, right, 8:12, :] = halo(even_x, c0[rs, 0:LANES], c1[rs, 0:LANES], have_right)
    lane = lax.broadcasted_iota(jnp.int32, (PACKED, LANES), 1)
    none = jnp.zeros((PACKED, LANES), jnp.float32)
    a, b = c0[:, LANES:], c1[:, LANES:]
    from_left = jnp.where(have_left, jnp.where(even_x, b, a), none)
    from_right = jnp.where(have_right, jnp.where(even_x, a, b), none)
    for g in range(6):
        l = pltpu.roll(from_left, LANES - 4 - 4 * g, 1)
        r = pltpu.roll(from_right, (LANES - 4 * g) % LANES, 1)
        both = jnp.where(lane < 4, r, jnp.where(lane >= LANES - 4, l, 0.0))
        strip, first = ((top, 4 * g) if g < 3 else (bottom, 4 * (g - 3)))
        for f in range(FIELDS):
            wide[f, strip + ntile, first : first + 4, :] = both[4 * f : 4 * f + 4, :]

    tiles = list(range(2 * group + 2))
    west, east = list(tiles), list(tiles)
    for first in (top, bottom):
        for t in range(group):
            west[first + t] = first + (t - 1) % group
            east[first + t] = first + (t + 1) % group
    base = base_ref[0]
    for t in tiles:
        order = plain_order if t < left else swapped_order
        for r in range(2):
            rs = pl.ds(8 * r, 8)
            kappa = wide[1, t, rs, :]
            store_members(s.mk, wide[0, t, rs, :].astype(jnp.int32), kappa, t, rs, order)
            s.raw[0, t, rs, :] = kappa
            for f in range(2, FIELDS):
                s.raw[f - 1, t, rs, :] = wide[f, t, rs, :]
    def run(pick):
        w = [pick.index(west[t]) for t in pick]
        e = [pick.index(east[t]) for t in pick]
        stage_share(s, pick, w, e, base + 1)
        stage_share(s, pick, w, e, base + 9)
        stage_average(s, pick, base + 2)
        stage_horizontal(s, pick, w, e, base + 2)
        stage_slope(s, pick, base + 3)
        return stage_push(s, pick, w, e, base + 4)

    made = run([left, right])
    turn[...] = jnp.zeros_like(turn)
    for f in range(3):
        fe = (0, 2, 1)[f]
        turn[pl.ds(4 * f, 4), :] = made[fe][0][0:4]
        turn[pl.ds(16 + 4 * f, 4), :] = made[fe][1][0:4]
    back = turn[...].T
    lane = lax.broadcasted_iota(jnp.int32, (rows, LANES), 1)
    for f in range(3):
        left_cols = pltpu.roll(back, (LANES - 4 * f) % LANES, 1)
        right_cols = pltpu.roll(back, LANES - 4 - 16 - 4 * f, 1)
        edge_c[0, f] = jnp.where(lane < 4, left_cols, inner_out[f, :, 0:LANES])
        edge_c[1, f] = jnp.where(lane >= LANES - 4, right_cols, inner_out[f, :, cols - LANES :])
    for i, col in enumerate((0, cols - LANES)):
        writes.append(
            pltpu.make_async_copy(
                edge_c.at[i, :, inside], out.at[:, inside, pl.ds(col, LANES)], sem.at[1 + i]
            )
        )
        writes[-1].start()
    for i, (strip, row) in enumerate(((top, 0), (bottom, rows - 8))):
        made = run(list(range(strip, strip + group)))
        fresh = slice(0, 4) if i == 0 else slice(4, 8)
        kept = slice(4, 8) if i == 0 else slice(0, 4)
        rs = slice(row + kept.start, row + kept.stop)
        for f in range(3):
            for t in range(ntile):
                ls = pl.ds(t * LANES, LANES)
                edge_r[i, f, fresh, ls] = made[f][t][0:4]
                if t in (0, ntile - 1):
                    edge_r[i, f, kept, ls] = edge_c[min(t, 1), f, rs]
                else:
                    edge_r[i, f, kept, ls] = inner_out[f, rs, ls]
        writes.append(pltpu.make_async_copy(edge_r.at[i], out.at[:, pl.ds(row, 8)], sem.at[3 + i]))
        writes[-1].start()
    for copy in writes:
        copy.wait()


def rim(h0, h1, c0, c1, own_rows, own_cols, inner_out):
    _, rows, cols = inner_out.shape
    ntile = cols // LANES
    tiles = 2 * (ntile + 1) + 2
    f32 = jnp.float32
    return pl.pallas_call(
        rim_kernel,
        out_shape=pltpu.HBM((3, rows, cols), f32),
        in_specs=[VMEM_SPEC] * 6 + [SMEM_SPEC, VMEM_SPEC],
        out_specs=HBM_SPEC,
        scratch_shapes=[pltpu.VMEM((FIELDS, tiles, 16, LANES), f32)]
        + Fields.shapes(tiles, 24)
        + [
            pltpu.VMEM((LANES, LANES), f32),
            pltpu.VMEM((2, 3, rows, LANES), f32),
            pltpu.VMEM((2, 3, 8, cols), f32),
            pltpu.SemaphoreType.DMA((5,)),
        ],
        compiler_params=pltpu.CompilerParams(vmem_limit_bytes=16 * MIB),
        cost_estimate=pl.CostEstimate(flops=10_000_000, transcendentals=0, bytes_accessed=1_000_000),
        name="rim",
    )(h0, h1, c0, c1, own_rows, own_cols, jnp.zeros((1,), jnp.int32), inner_out)


def corner_kernel(h0, h1, p0, p1, q0, q1):
    iy, ix = lax.axis_index("ty"), lax.axis_index("tx")
    even_y, even_x = lax.rem(iy, 2) == 0, lax.rem(ix, 2) == 0
    have_top, have_bottom = iy > 0, iy < lax.axis_size("ty") - 1
    cols = h0.shape[1]
    lane = lax.broadcasted_iota(jnp.int32, (PACKED, LANES), 1)
    corners = []
    for first, ls in ((0, pl.ds(0, LANES)), (LANES - 4, pl.ds(cols - LANES, LANES))):
        a, b = h0[:, ls], h1[:, ls]
        above = jnp.where(have_top, jnp.where(even_y, b, a), 0.0)
        below = jnp.where(have_bottom, jnp.where(even_y, a, b), 0.0)
        above = pltpu.roll(above, (LANES - first) % LANES, 1)
        below = pltpu.roll(below, (20 + LANES - first) % LANES, 1)
        total = jnp.where(lane < 4, above, 0.0)
        corners.append(jnp.where((lane >= 20) & (lane < 24), below, total))
    left, right = corners
    q0[:, 0:LANES] = p0[:, 0:LANES]
    q1[:, 0:LANES] = p1[:, 0:LANES]
    q0[:, LANES:] = p0[:, LANES:] + jnp.where(even_x, right, left)
    q1[:, LANES:] = p1[:, LANES:] + jnp.where(even_x, left, right)


def with_corners(h0, h1, p0, p1):
    return pl.pallas_call(
        corner_kernel,
        out_shape=(pltpu.VMEM(p0.shape, jnp.float32), pltpu.VMEM(p1.shape, jnp.float32)),
        in_specs=[VMEM_SPEC] * 4,
        out_specs=[VMEM_SPEC] * 2,
        compiler_params=pltpu.CompilerParams(vmem_limit_bytes=2 * MIB),
        name="corner",
    )(h0, h1, p0, p1)


def body(state, cut_mask, fraction, neighbourhood, tile_flags, centroid_offset):
    args = (state, cut_mask, fraction, neighbourhood, tile_flags, centroid_offset)
    s0, s1, own_rows, limit = pack(*args)
    h0 = in_vmem(paired(s0, "ty", "tx", 0))
    h1 = in_vmem(paired(s1, "ty", "tx", 1))
    held = [in_vmem(a) for a in (state, cut_mask, fraction, neighbourhood, centroid_offset)]
    p0, p1, own_cols, *fields = first_part(*held, limit, own_rows)
    q0, q1 = with_corners(h0, h1, p0, p1)
    c0 = in_vmem(paired(q0, "tx", "ty", 0))
    c1 = in_vmem(paired(q1, "tx", "ty", 1))
    inner_out = second_part(state.shape[1], *fields)
    return rim(h0, h1, c0, c1, own_rows, own_cols, inner_out)


def solution(mesh):
    placed = (
        P(None, "ty", "tx"),
        P("ty", "tx"),
        P("ty", "tx"),
        P("ty", "tx"),
        P("ty", "tx"),
        P(None, "ty", "tx"),
    )
    return jax.shard_map(
        body, mesh=mesh, in_specs=placed, out_specs=P(None, "ty", "tx"), check_vma=False
    )
```

```python
import functools

import jax
import jax.numpy as jnp
from jax import lax
from jax.experimental import pallas as pl
from jax.experimental.pallas import tpu as pltpu
from jax.sharding import PartitionSpec as P

DEPTH = 4
LANES = 128
FIELDS = 7
PACKED = 4 * FIELDS
MIB = 1024 * 1024
ORIGIN = 8

courant = 0.1


def paired(value, axis, other, first):
    length, width = lax.axis_size(axis), lax.axis_size(other)
    pairs = []
    for i in range(length):
        for j in range(width):
            mate = (i + 1 if (i - first) % 2 == 0 else i - 1, j)
            if not 0 <= mate[0] < length:
                mate = (i, j ^ 1)
            here = i * width + j
            there = mate[0] * width + mate[1]
            pairs.append((here, there))
    if axis == "tx":
        swap = lambda k: (k % width) * length + k // width
        pairs = [(swap(a), swap(b)) for a, b in pairs]
    return lax.ppermute(value, ("ty", "tx"), sorted(pairs))


def lane_index():
    return lax.broadcasted_iota(jnp.int32, (8, LANES), 1)


def from_west(values, west, lane):
    return [
        pltpu.roll(jnp.where(lane == LANES - 1, values[west[t]], values[t]), 1, 1)
        for t in range(len(values))
    ]


def from_east(values, east, lane):
    return [
        pltpu.roll(jnp.where(lane == 0, values[east[t]], values[t]), LANES - 1, 1)
        for t in range(len(values))
    ]


def inverse(value):
    guess = pl.reciprocal(value, approx=True)
    return guess * (2.0 - value * guess)


def store_members(mk, code, kappa, t, rows, order):
    for b in range(9):
        held = (code & (1 << order[b])) != 0
        mk[b, t, rows, :] = jnp.where(held, kappa, 0.0)


plain_order = (0, 1, 2, 3, 4, 5, 6, 7, 8)
swapped_order = (0, 3, 6, 1, 4, 7, 2, 5, 8)


class Fields:
    def __init__(self, mk, raw, rc, seen, gath, cent, horiz, push):
        self.mk, self.raw, self.rc, self.seen = mk, raw, rc, seen
        self.gath, self.cent, self.horiz, self.push = gath, cent, horiz, push

    @staticmethod
    def shapes(tiles, rows):
        shape = lambda n: pltpu.VMEM((n, tiles, rows, LANES), jnp.float32)
        return [shape(9), shape(6), shape(1), shape(4), shape(18), shape(5), shape(14), shape(9)]


def at(ref, i, t, base, step=0):
    return ref[i, t, pl.ds(base + step, 8), :]


def stage_share(s, tiles, west, east, base):
    lane = lane_index()
    n = len(tiles)
    sums = []
    for dx in (-1, 0, 1):
        group = []
        for t in tiles:
            total = at(s.mk, 4 + dx, t, base)
            total = total + at(s.mk, 1 + dx, t, base, 1)
            total = total + at(s.mk, 7 + dx, t, base, -1)
            group.append(total)
        sums.append(group)
    low = from_east(sums[0], east, lane)
    high = from_west(sums[2], west, lane)
    centre = [[at(s.raw, 3 + f, t, base) for t in tiles] for f in range(3)]
    easts = [from_east(c, east, lane) for c in centre]
    wests = [from_west(c, west, lane) for c in centre]
    for i, move, step in ((0, from_west, -1.0), (1, from_east, 1.0)):
        beside = west if i == 0 else east
        x = move([at(s.raw, 1, t, base) for t in tiles], beside, lane)
        y = move([at(s.raw, 2, t, base) for t in tiles], beside, lane)
        for k, t in enumerate(tiles):
            s.seen[i, t, pl.ds(base, 8), :] = x[k] + step
            s.seen[2 + i, t, pl.ds(base, 8), :] = y[k]
    outs = [[] for _ in range(6)]
    for k, t in enumerate(tiles):
        coverage = jnp.maximum(sums[1][k] + low[k] + high[k], 0.125)
        rc = inverse(coverage)
        s.rc[0, t, pl.ds(base, 8), :] = rc
        share = at(s.raw, 0, t, base) * rc
        rate = (0.5 * courant) * rc
        keep = share - 4.0 * rate
        c = [centre[f][k] for f in range(3)]
        e = [easts[f][k] for f in range(3)]
        w = [wests[f][k] for f in range(3)]
        north = [at(s.raw, 3 + f, t, base, 1) for f in range(3)]
        south = [at(s.raw, 3 + f, t, base, -1) for f in range(3)]
        flux = [(e[1] - w[1]) + (north[2] - south[2]), e[0] - w[0], north[0] - south[0]]
        outs[0].append(share)
        outs[1].append(share * at(s.raw, 1, t, base))
        outs[2].append(share * at(s.raw, 2, t, base))
        for f in range(3):
            around = (e[f] + w[f]) + (north[f] + south[f])
            outs[3 + f].append(keep * c[f] - rate * (flux[f] - around))
    for f in range(6):
        w = from_west(outs[f], west, lane)
        e = from_east(outs[f], east, lane)
        for k, t in enumerate(tiles):
            s.gath[3 * f, t, pl.ds(base, 8), :] = w[k]
            s.gath[3 * f + 1, t, pl.ds(base, 8), :] = outs[f][k]
            s.gath[3 * f + 2, t, pl.ds(base, 8), :] = e[k]


def stage_average(s, tiles, base):
    for t in tiles:
        weight = {}
        for dy in (-1, 0, 1):
            for dx in (-1, 0, 1):
                member = at(s.mk, 3 * (dy + 1) + dx + 1, t, base)
                weight[dy, dx] = (member, member * at(s.gath, 1 + dx, t, base, dy))
        cols = [weight[-1, d][1] + weight[0, d][1] + weight[1, d][1] for d in (-1, 0, 1)]
        total = cols[0] + cols[1] + cols[2]
        upper = weight[1, -1][1] + weight[1, 0][1] + weight[1, 1][1]
        lower = weight[-1, -1][1] + weight[-1, 0][1] + weight[-1, 1][1]
        sums = [cols[2] - cols[0], upper - lower, None, None, None]
        for f in range(5):
            for dy in (-1, 0, 1):
                for dx in (-1, 0, 1):
                    term = weight[dy, dx][0] * at(s.gath, 3 * (f + 1) + 1 + dx, t, base, dy)
                    sums[f] = term if sums[f] is None else sums[f] + term
        inv = inverse(jnp.maximum(total, 1e-3))
        for f in range(5):
            s.cent[f, t, pl.ds(base, 8), :] = sums[f] * inv


def stage_horizontal(s, tiles, west, east, base):
    lane = lane_index()
    results = [[at(s.cent, f, t, base) for t in tiles] for f in range(5)]
    w = [from_west(r, west, lane) for r in results]
    e = [from_east(r, east, lane) for r in results]
    for k, t in enumerate(tiles):
        x = [w[0][k] - 1.0, results[0][k], e[0][k] + 1.0]
        v = [w[1][k], results[1][k], e[1][k]]
        a = [[w[2 + f][k], results[2 + f][k], e[2 + f][k]] for f in range(3)]
        add3 = lambda p: p[0] + p[1] + p[2]
        dot3 = lambda p, q: p[0] * q[0] + p[1] * q[1] + p[2] * q[2]
        made = [add3(x), add3(v), dot3(x, x), dot3(x, v), dot3(v, v)]
        made += [add3(a[f]) for f in range(3)]
        made += [dot3(x, a[f]) for f in range(3)]
        made += [dot3(v, a[f]) for f in range(3)]
        for i, value in enumerate(made):
            s.horiz[i, t, pl.ds(base, 8), :] = value


def stage_slope(s, tiles, base):
    for t in tiles:
        rows = lambda i: [at(s.horiz, i, t, base, d) for d in (-1, 0, 1)]
        add3 = lambda p: p[0] + p[1] + p[2]
        u, v = at(s.cent, 0, t, base), at(s.cent, 1, t, base)
        hx, hv = rows(0), rows(1)
        sum_x, sum_y = add3(hx), add3(hv)
        sum_xx = add3(rows(2)) + 1.0
        sum_xy = add3(rows(3)) + (hx[2] - hx[0])
        sum_yy = add3(rows(4)) + (2.0 * (hv[2] - hv[0]) + 7.0)
        mean_x = sum_x - 9.0 * u
        mean_y = sum_y - 9.0 * v
        moment_xx = sum_xx - u * (sum_x + mean_x)
        moment_yy = sum_yy - v * (sum_y + mean_y)
        moment_xy = sum_xy - u * sum_y - v * mean_x
        inv = inverse(moment_xx * moment_yy - moment_xy * moment_xy)
        moment_xx = moment_xx * inv
        moment_yy = moment_yy * inv
        moment_xy = moment_xy * inv
        for f in range(3):
            average = at(s.cent, 2 + f, t, base)
            ha = rows(5 + f)
            sum_a = add3(ha)
            right_x = add3(rows(8 + f)) - u * sum_a - average * mean_x
            right_y = add3(rows(11 + f)) + (ha[2] - ha[0]) - v * sum_a - average * mean_y
            slope_x = moment_yy * right_x - moment_xy * right_y
            slope_y = moment_xx * right_y - moment_xy * right_x
            s.push[f, t, pl.ds(base, 8), :] = average - slope_x * u - slope_y * v
            s.push[3 + f, t, pl.ds(base, 8), :] = slope_x
            s.push[6 + f, t, pl.ds(base, 8), :] = slope_y


def stage_push(s, tiles, west, east, base):
    lane = lane_index()
    groups = [[[] for _ in range(3)] for _ in range(3)]
    for t in tiles:
        for dx in (-1, 0, 1):
            if dx:
                x, middle = at(s.seen, (dx + 1) // 2, t, base), at(s.seen, 2 + (dx + 1) // 2, t, base)
            else:
                x, middle = at(s.raw, 1, t, base), at(s.raw, 2, t, base)
            totals = [None] * 3
            for dy in (-1, 0, 1):
                y = middle + float(dy) if dy else middle
                member = at(s.mk, 3 * (dy + 1) + dx + 1, t, base, -dy)
                for f in range(3):
                    plane = at(s.push, f, t, base, -dy)
                    plane = plane + at(s.push, 3 + f, t, base, -dy) * x
                    plane = plane + at(s.push, 6 + f, t, base, -dy) * y
                    term = member * plane
                    totals[f] = term if totals[f] is None else totals[f] + term
            for f in range(3):
                groups[dx + 1][f].append(totals[f])
    results = []
    for f in range(3):
        low = from_east(groups[0][f], east, lane)
        high = from_west(groups[2][f], west, lane)
        results.append(
            [
                (groups[1][f][k] + low[k] + high[k]) * at(s.rc, 0, t, base)
                for k, t in enumerate(tiles)
            ]
        )
    return results


def start_all(copies):
    for copy in copies:
        copy.start()
    for copy in copies:
        copy.wait()


def strip_fields(state, cut, fraction, code, offset, rs, ls, limit):
    active = cut[rs, ls] > limit
    return [
        jnp.where(active, code[rs, ls], 16).astype(jnp.float32),
        jnp.where(active, fraction[rs, ls].astype(jnp.float32) * (1.0 / 1024.0), 1.0),
        jnp.where(active, offset[0, rs, ls], 0.0),
        jnp.where(active, offset[1, rs, ls], 0.0),
        state[0, rs, ls],
        state[1, rs, ls],
        state[2, rs, ls],
    ]


def pack_kernel(
    state_in, cut_in, fraction_in, code_in, flags_in, offset_in,
    s0, s1, own_rows, limit, state, cut, fraction, code, offset, flags, sem,
):
    rows, cols = cut_in.shape
    copies = [pltpu.make_async_copy(flags_in, flags, sem.at[2, 0])]
    for i in range(2):
        rs, to = pl.ds(i * (rows - 8), 8), pl.ds(8 * i, 8)
        pairs = [
            (cut_in.at[rs], cut.at[to]),
            (code_in.at[rs], code.at[to]),
            (fraction_in.at[rs], fraction.at[to]),
            (offset_in.at[:, rs], offset.at[:, to]),
            (state_in.at[:, rs], state.at[:, to]),
        ]
        copies += [pltpu.make_async_copy(a, b, sem.at[i, j]) for j, (a, b) in enumerate(pairs)]
    start_all(copies)
    even_y = lax.rem(lax.axis_index("ty"), 2) == 0
    for t in range(cols // LANES):
        ls = pl.ds(t * LANES, LANES)
        level = 1 - flags[0, t]
        limit[:, ls] = jnp.full((8, LANES), level, jnp.int32)
        made = []
        for i in range(2):
            got = strip_fields(state, cut, fraction, code, offset, pl.ds(8 * i, 8), ls, level)
            for f in range(FIELDS):
                own_rows[i, f, :, ls] = got[f]
            made.append(got)
        for f in range(FIELDS):
            top = made[0][f][0:4]
            bottom = made[1][f][4:8]
            s0[pl.ds(4 * f, 4), ls] = jnp.where(even_y, bottom, top)
            s1[pl.ds(4 * f, 4), ls] = jnp.where(even_y, top, bottom)


def in_vmem(value):
    return pltpu.with_memory_space_constraint(value, pltpu.VMEM)


def in_hbm(value):
    return pltpu.with_memory_space_constraint(value, pltpu.HBM)


VMEM_SPEC = pl.BlockSpec(memory_space=pltpu.VMEM)
SMEM_SPEC = pl.BlockSpec(memory_space=pltpu.SMEM)
HBM_SPEC = pl.BlockSpec(memory_space=pltpu.HBM)


def pack(*args):
    cols = args[1].shape[1]
    f32, i32 = jnp.float32, jnp.int32
    made = pl.pallas_call(
        pack_kernel,
        out_shape=(
            pltpu.VMEM((PACKED, cols), f32), pltpu.VMEM((PACKED, cols), f32),
            pltpu.VMEM((2, FIELDS, 8, cols), f32), pltpu.VMEM((8, cols), i32),
        ),
        in_specs=[HBM_SPEC] * 6,
        out_specs=[VMEM_SPEC] * 4,
        scratch_shapes=[
            pltpu.VMEM((3, 16, cols), f32),
            pltpu.VMEM((16, cols), i32),
            pltpu.VMEM((16, cols), i32),
            pltpu.VMEM((16, cols), i32),
            pltpu.VMEM((2, 16, cols), f32),
            pltpu.SMEM((1, cols // LANES), i32),
            pltpu.SemaphoreType.DMA((3, 5)),
        ],
        compiler_params=pltpu.CompilerParams(vmem_limit_bytes=2 * MIB),
        name="pack",
    )(*[in_hbm(a) for a in args])
    return [in_vmem(m) for m in made]


def first_kernel(
    state, cut, fraction, code, offset, limit, own_rows, p0, p1, own_cols, mk, raw, rc, seen, cent, gath, mix
):
    s = Fields(mk, raw, rc, seen, gath, cent, None, None)
    rows, cols = cut.shape
    ntile = cols // LANES
    tiles = list(range(ntile))
    west = [(t - 1) % ntile for t in tiles]
    east = [(t + 1) % ntile for t in tiles]

    even_x = lax.rem(lax.axis_index("tx"), 2) == 0
    for side, t in enumerate((0, ntile - 1)):
        ls = pl.ds(t * LANES, LANES)
        got = strip_fields(state, cut, fraction, code, offset, slice(None), ls, limit[0:1, ls])
        first = 0 if side == 0 else LANES - 8
        for f in range(FIELDS):
            own_cols[side, f, :, :] = got[f].T[first : first + 8, :]
    for f in range(FIELDS):
        left = own_cols[0, f, 0:4, :]
        right = own_cols[1, f, 4:8, :]
        rs = pl.ds(4 * f, 4)
        p0[rs, 0:LANES] = jnp.where(even_x, right, left)
        p1[rs, 0:LANES] = jnp.where(even_x, left, right)
        for side in range(2):
            ls = pl.ds(side * (cols - LANES), LANES)
            first = 0 if side == 0 else LANES - 4
            near, far = own_rows[0, f, :, ls], own_rows[1, f, :, ls]
            for g, piece in ((1, near[0:4]), (2, near[4:8]), (3, far[0:4]), (4, far[4:8])):
                mix[side, g, rs, :] = pltpu.roll(piece, (4 * g - first) % LANES, 1)
    lane = lax.broadcasted_iota(jnp.int32, (PACKED, LANES), 1)
    parts = []
    for side in range(2):
        total = jnp.zeros((PACKED, LANES), jnp.float32)
        for g in range(1, 5):
            here = (lane >= 4 * g) & (lane < 4 * g + 4)
            total = jnp.where(here, mix[side, g, 0:PACKED, :], total)
        parts.append(total)
    p0[:, LANES:] = jnp.where(even_x, parts[1], parts[0])
    p1[:, LANES:] = jnp.where(even_x, parts[0], parts[1])

    def prepare(k, carry):
        src = pl.ds(pl.multiple_of(8 * k, 8), 8)
        dst = pl.ds(pl.multiple_of(8 * k + ORIGIN, 8), 8)
        for t in tiles:
            ls = pl.ds(t * LANES, LANES)
            active = cut[src, ls] > limit[:, ls]
            codes = jnp.where(active, code[src, ls], 16)
            kappa = jnp.where(active, fraction[src, ls].astype(jnp.float32) * (1.0 / 1024.0), 1.0)
            s.raw[0, t, dst, :] = kappa
            for i in range(2):
                s.raw[1 + i, t, dst, :] = jnp.where(active, offset[i, src, ls], 0.0)
            for f in range(3):
                s.raw[3 + f, t, dst, :] = state[f, src, ls]
            store_members(s.mk, codes, kappa, t, dst, plain_order)
        return carry

    def sweep(k, carry):
        stage_share(s, tiles, west, east, 8 * k + ORIGIN)
        return carry

    def sweep2(k, carry):
        stage_average(s, tiles, 8 * k + ORIGIN)
        return carry

    lax.fori_loop(0, rows // 8, prepare, 0)
    lax.fori_loop(0, rows // 8, sweep, 0)
    lax.fori_loop(0, rows // 8, sweep2, 0)


def second_kernel(mk, raw, rc, seen, cent, out, horiz, push):
    s = Fields(mk, raw, rc, seen, None, cent, horiz, push)
    ntile = mk.shape[1]
    count = out.shape[1] // 8
    tiles = list(range(ntile))
    west = [(t - 1) % ntile for t in tiles]
    east = [(t + 1) % ntile for t in tiles]

    def slopes(k, carry):
        stage_horizontal(s, tiles, west, east, 8 * k + ORIGIN)
        return carry

    def slopes2(k, carry):
        stage_slope(s, tiles, 8 * k + ORIGIN)
        return carry

    def spread(k, carry):
        made = stage_push(s, tiles, west, east, 8 * k + ORIGIN)
        for f in range(3):
            for t in tiles:
                out[f, pl.ds(pl.multiple_of(8 * k, 8), 8), pl.ds(t * LANES, LANES)] = made[f][t]
        return carry

    lax.fori_loop(0, count, slopes, 0)
    lax.fori_loop(0, count, slopes2, 0)
    lax.fori_loop(0, count, spread, 0)


def first_part(state, cut, fraction, code, offset, limit, own_rows):
    rows, cols = cut.shape
    ntile = cols // LANES
    f32 = jnp.float32
    mk, raw, rc, seen, _, cent, _, _ = Fields.shapes(ntile, rows + 16)
    gath = Fields.shapes(ntile + 1, rows + 24)[4]
    made = pl.pallas_call(
        first_kernel,
        out_shape=(
            pltpu.VMEM((PACKED, 2 * LANES), f32), pltpu.VMEM((PACKED, 2 * LANES), f32),
            pltpu.VMEM((2, FIELDS, 8, rows), f32), mk, raw, rc, seen, cent,
        ),
        in_specs=[VMEM_SPEC] * 7,
        out_specs=[VMEM_SPEC] * 8,
        scratch_shapes=[gath, pltpu.VMEM((2, 5, 32, LANES), f32)],
        compiler_params=pltpu.CompilerParams(vmem_limit_bytes=10 * MIB),
        cost_estimate=pl.CostEstimate(flops=30_000_000, transcendentals=0, bytes_accessed=1_000_000),
        name="first",
    )(state, cut, fraction, code, offset, limit, own_rows)
    return [in_vmem(m) for m in made]


def second_part(rows, *held):
    ntile = held[0].shape[1]
    *_, horiz, push = Fields.shapes(ntile + 1, rows + 24)
    return in_vmem(
        pl.pallas_call(
            second_kernel,
            out_shape=pltpu.VMEM((3, rows, ntile * LANES), jnp.float32),
            in_specs=[VMEM_SPEC] * 5,
            out_specs=VMEM_SPEC,
            scratch_shapes=[horiz, push],
            compiler_params=pltpu.CompilerParams(vmem_limit_bytes=12 * MIB),
            cost_estimate=pl.CostEstimate(flops=30_000_000, transcendentals=0, bytes_accessed=1_000_000),
            name="second",
        )(*held)
    )


swap_fields = (0, 1, 3, 2, 4, 6, 5)


def rim_kernel(h0, h1, c0, c1, own_rows, own_cols, base_ref, inner_out, out, wide, *rest):
    s = Fields(*rest[:8])
    turn, edge_c, edge_r, sem = rest[8:]
    _, rows, cols = out.shape
    ntile = cols // LANES
    inside = pl.ds(8, rows - 16)
    middle = pl.ds(LANES, cols - 2 * LANES)
    writes = [pltpu.make_async_copy(inner_out.at[:, inside, middle], out.at[:, inside, middle], sem.at[0])]
    writes[0].start()
    iy, ix = lax.axis_index("ty"), lax.axis_index("tx")
    even_y, even_x = lax.rem(iy, 2) == 0, lax.rem(ix, 2) == 0
    have_top, have_bottom = iy > 0, iy < lax.axis_size("ty") - 1
    have_left, have_right = ix > 0, ix < lax.axis_size("tx") - 1
    group = ntile + 1
    top, bottom, left, right = 0, group, 2 * group, 2 * group + 1
    zero4 = jnp.zeros((4, LANES), jnp.float32)
    halo = lambda even, a, b, have: jnp.where(have, jnp.where(even, a, b), zero4)
    for f in range(FIELDS):
        rs = pl.ds(4 * f, 4)
        for t in range(ntile):
            ls = pl.ds(t * LANES, LANES)
            wide[f, top + t, 0:4, :] = halo(even_y, h1[rs, ls], h0[rs, ls], have_top)
            wide[f, top + t, 4:12, :] = own_rows[0, f, :, ls]
            wide[f, bottom + t, 0:8, :] = own_rows[1, f, :, ls]
            wide[f, bottom + t, 8:12, :] = halo(even_y, h0[rs, ls], h1[rs, ls], have_bottom)
        fe = swap_fields[f]
        wide[fe, left, 0:4, :] = halo(even_x, c1[rs, 0:LANES], c0[rs, 0:LANES], have_left)
        wide[fe, left, 4:12, :] = own_cols[0, f, :, :]
        wide[fe, right, 0:8, :] = own_cols[1, f, :, :]
        wide[fe, right, 8:12, :] = halo(even_x, c0[rs, 0:LANES], c1[rs, 0:LANES], have_right)
    lane = lax.broadcasted_iota(jnp.int32, (PACKED, LANES), 1)
    none = jnp.zeros((PACKED, LANES), jnp.float32)
    a, b = c0[:, LANES:], c1[:, LANES:]
    from_left = jnp.where(have_left, jnp.where(even_x, b, a), none)
    from_right = jnp.where(have_right, jnp.where(even_x, a, b), none)
    for g in range(6):
        l = pltpu.roll(from_left, LANES - 4 - 4 * g, 1)
        r = pltpu.roll(from_right, (LANES - 4 * g) % LANES, 1)
        both = jnp.where(lane < 4, r, jnp.where(lane >= LANES - 4, l, 0.0))
        strip, first = ((top, 4 * g) if g < 3 else (bottom, 4 * (g - 3)))
        for f in range(FIELDS):
            wide[f, strip + ntile, first : first + 4, :] = both[4 * f : 4 * f + 4, :]

    tiles = list(range(2 * group + 2))
    west, east = list(tiles), list(tiles)
    for first in (top, bottom):
        for t in range(group):
            west[first + t] = first + (t - 1) % group
            east[first + t] = first + (t + 1) % group
    base = base_ref[0]
    for t in tiles:
        order = plain_order if t < left else swapped_order
        for r in range(2):
            rs = pl.ds(8 * r, 8)
            kappa = wide[1, t, rs, :]
            store_members(s.mk, wide[0, t, rs, :].astype(jnp.int32), kappa, t, rs, order)
            s.raw[0, t, rs, :] = kappa
            for f in range(2, FIELDS):
                s.raw[f - 1, t, rs, :] = wide[f, t, rs, :]
    def run(pick):
        w = [pick.index(west[t]) for t in pick]
        e = [pick.index(east[t]) for t in pick]
        stage_share(s, pick, w, e, base + 1)
        stage_share(s, pick, w, e, base + 9)
        stage_average(s, pick, base + 2)
        stage_horizontal(s, pick, w, e, base + 2)
        stage_slope(s, pick, base + 3)
        return stage_push(s, pick, w, e, base + 4)

    made = run([left, right])
    turn[...] = jnp.zeros_like(turn)
    for f in range(3):
        fe = (0, 2, 1)[f]
        turn[pl.ds(4 * f, 4), :] = made[fe][0][0:4]
        turn[pl.ds(16 + 4 * f, 4), :] = made[fe][1][0:4]
    back = turn[...].T
    lane = lax.broadcasted_iota(jnp.int32, (rows, LANES), 1)
    for f in range(3):
        left_cols = pltpu.roll(back, (LANES - 4 * f) % LANES, 1)
        right_cols = pltpu.roll(back, LANES - 4 - 16 - 4 * f, 1)
        edge_c[0, f] = jnp.where(lane < 4, left_cols, inner_out[f, :, 0:LANES])
        edge_c[1, f] = jnp.where(lane >= LANES - 4, right_cols, inner_out[f, :, cols - LANES :])
    for i, col in enumerate((0, cols - LANES)):
        writes.append(
            pltpu.make_async_copy(
                edge_c.at[i, :, inside], out.at[:, inside, pl.ds(col, LANES)], sem.at[1 + i]
            )
        )
        writes[-1].start()
    for i, (strip, row) in enumerate(((top, 0), (bottom, rows - 8))):
        made = run(list(range(strip, strip + group)))
        fresh = slice(0, 4) if i == 0 else slice(4, 8)
        kept = slice(4, 8) if i == 0 else slice(0, 4)
        rs = slice(row + kept.start, row + kept.stop)
        for f in range(3):
            for t in range(ntile):
                ls = pl.ds(t * LANES, LANES)
                edge_r[i, f, fresh, ls] = made[f][t][0:4]
                if t in (0, ntile - 1):
                    edge_r[i, f, kept, ls] = edge_c[min(t, 1), f, rs]
                else:
                    edge_r[i, f, kept, ls] = inner_out[f, rs, ls]
        writes.append(pltpu.make_async_copy(edge_r.at[i], out.at[:, pl.ds(row, 8)], sem.at[3 + i]))
        writes[-1].start()
    for copy in writes:
        copy.wait()


def rim(h0, h1, c0, c1, own_rows, own_cols, inner_out):
    _, rows, cols = inner_out.shape
    ntile = cols // LANES
    tiles = 2 * (ntile + 1) + 2
    f32 = jnp.float32
    return pl.pallas_call(
        rim_kernel,
        out_shape=pltpu.HBM((3, rows, cols), f32),
        in_specs=[VMEM_SPEC] * 6 + [SMEM_SPEC, VMEM_SPEC],
        out_specs=HBM_SPEC,
        scratch_shapes=[pltpu.VMEM((FIELDS, tiles + 1, 24, LANES), f32)]
        + Fields.shapes(tiles + 1, 24)
        + [
            pltpu.VMEM((LANES, LANES), f32),
            pltpu.VMEM((2, 3, rows, LANES), f32),
            pltpu.VMEM((2, 3, 8, cols), f32),
            pltpu.SemaphoreType.DMA((5,)),
        ],
        compiler_params=pltpu.CompilerParams(vmem_limit_bytes=16 * MIB),
        cost_estimate=pl.CostEstimate(flops=10_000_000, transcendentals=0, bytes_accessed=1_000_000),
        name="rim",
    )(h0, h1, c0, c1, own_rows, own_cols, jnp.zeros((1,), jnp.int32), inner_out)


def corner_kernel(h0, h1, p0, p1, q0, q1):
    iy, ix = lax.axis_index("ty"), lax.axis_index("tx")
    even_y, even_x = lax.rem(iy, 2) == 0, lax.rem(ix, 2) == 0
    have_top, have_bottom = iy > 0, iy < lax.axis_size("ty") - 1
    cols = h0.shape[1]
    lane = lax.broadcasted_iota(jnp.int32, (PACKED, LANES), 1)
    corners = []
    for first, ls in ((0, pl.ds(0, LANES)), (LANES - 4, pl.ds(cols - LANES, LANES))):
        a, b = h0[:, ls], h1[:, ls]
        above = jnp.where(have_top, jnp.where(even_y, b, a), 0.0)
        below = jnp.where(have_bottom, jnp.where(even_y, a, b), 0.0)
        above = pltpu.roll(above, (LANES - first) % LANES, 1)
        below = pltpu.roll(below, (20 + LANES - first) % LANES, 1)
        total = jnp.where(lane < 4, above, 0.0)
        corners.append(jnp.where((lane >= 20) & (lane < 24), below, total))
    left, right = corners
    q0[:, 0:LANES] = p0[:, 0:LANES]
    q1[:, 0:LANES] = p1[:, 0:LANES]
    q0[:, LANES:] = p0[:, LANES:] + jnp.where(even_x, right, left)
    q1[:, LANES:] = p1[:, LANES:] + jnp.where(even_x, left, right)


def with_corners(h0, h1, p0, p1):
    return pl.pallas_call(
        corner_kernel,
        out_shape=(pltpu.VMEM(p0.shape, jnp.float32), pltpu.VMEM(p1.shape, jnp.float32)),
        in_specs=[VMEM_SPEC] * 4,
        out_specs=[VMEM_SPEC] * 2,
        compiler_params=pltpu.CompilerParams(vmem_limit_bytes=2 * MIB),
        name="corner",
    )(h0, h1, p0, p1)


def body(state, cut_mask, fraction, neighbourhood, tile_flags, centroid_offset):
    args = (state, cut_mask, fraction, neighbourhood, tile_flags, centroid_offset)
    s0, s1, own_rows, limit = pack(*args)
    h0 = in_vmem(paired(s0, "ty", "tx", 0))
    h1 = in_vmem(paired(s1, "ty", "tx", 1))
    held = [in_vmem(a) for a in (state, cut_mask, fraction, neighbourhood, centroid_offset)]
    p0, p1, own_cols, *fields = first_part(*held, limit, own_rows)
    q0, q1 = with_corners(h0, h1, p0, p1)
    c0 = in_vmem(paired(q0, "tx", "ty", 0))
    c1 = in_vmem(paired(q1, "tx", "ty", 1))
    inner_out = second_part(state.shape[1], *fields)
    return rim(h0, h1, c0, c1, own_rows, own_cols, inner_out)


def solution(mesh):
    placed = (
        P(None, "ty", "tx"),
        P("ty", "tx"),
        P("ty", "tx"),
        P("ty", "tx"),
        P("ty", "tx"),
        P(None, "ty", "tx"),
    )
    return jax.shard_map(
        body, mesh=mesh, in_specs=placed, out_specs=P(None, "ty", "tx"), check_vma=False
    )
```

```python
import functools

import jax
import jax.numpy as jnp
from jax import lax
from jax.experimental import pallas as pl
from jax.experimental.pallas import tpu as pltpu
from jax.sharding import PartitionSpec as P

DEPTH = 4
LANES = 128
FIELDS = 7
PACKED = 4 * FIELDS
MIB = 1024 * 1024
ORIGIN = 8

courant = 0.1


def paired(value, axis, other, first):
    length, width = lax.axis_size(axis), lax.axis_size(other)
    pairs = []
    for i in range(length):
        for j in range(width):
            mate = (i + 1 if (i - first) % 2 == 0 else i - 1, j)
            if not 0 <= mate[0] < length:
                mate = (i, j ^ 1)
            here = i * width + j
            there = mate[0] * width + mate[1]
            pairs.append((here, there))
    if axis == "tx":
        swap = lambda k: (k % width) * length + k // width
        pairs = [(swap(a), swap(b)) for a, b in pairs]
    return lax.ppermute(value, ("ty", "tx"), sorted(pairs))


def lane_index():
    return lax.broadcasted_iota(jnp.int32, (8, LANES), 1)


def from_west(values, west, lane):
    return [
        pltpu.roll(jnp.where(lane == LANES - 1, values[west[t]], values[t]), 1, 1)
        for t in range(len(values))
    ]


def from_east(values, east, lane):
    return [
        pltpu.roll(jnp.where(lane == 0, values[east[t]], values[t]), LANES - 1, 1)
        for t in range(len(values))
    ]


def inverse(value):
    guess = pl.reciprocal(value, approx=True)
    return guess * (2.0 - value * guess)


def store_members(mk, code, kappa, t, rows, order):
    for b in range(9):
        held = (code & (1 << order[b])) != 0
        mk[b, t, rows, :] = jnp.where(held, kappa, 0.0)


plain_order = (0, 1, 2, 3, 4, 5, 6, 7, 8)
swapped_order = (0, 3, 6, 1, 4, 7, 2, 5, 8)


class Fields:
    def __init__(self, mk, raw, rc, seen, gath, cent, horiz, push):
        self.mk, self.raw, self.rc, self.seen = mk, raw, rc, seen
        self.gath, self.cent, self.horiz, self.push = gath, cent, horiz, push

    @staticmethod
    def shapes(tiles, rows):
        shape = lambda n: pltpu.VMEM((n, tiles, rows, LANES), jnp.float32)
        return [shape(9), shape(6), shape(1), shape(4), shape(18), shape(5), shape(14), shape(9)]


def at(ref, i, t, base, step=0):
    return ref[i, t, pl.ds(base + step, 8), :]


def stage_share(s, tiles, west, east, base):
    lane = lane_index()
    n = len(tiles)
    sums = []
    for dx in (-1, 0, 1):
        group = []
        for t in tiles:
            total = at(s.mk, 4 + dx, t, base)
            total = total + at(s.mk, 1 + dx, t, base, 1)
            total = total + at(s.mk, 7 + dx, t, base, -1)
            group.append(total)
        sums.append(group)
    low = from_east(sums[0], east, lane)
    high = from_west(sums[2], west, lane)
    centre = [[at(s.raw, 3 + f, t, base) for t in tiles] for f in range(3)]
    easts = [from_east(c, east, lane) for c in centre]
    wests = [from_west(c, west, lane) for c in centre]
    for i, move, step in ((0, from_west, -1.0), (1, from_east, 1.0)):
        beside = west if i == 0 else east
        x = move([at(s.raw, 1, t, base) for t in tiles], beside, lane)
        y = move([at(s.raw, 2, t, base) for t in tiles], beside, lane)
        for k, t in enumerate(tiles):
            s.seen[i, t, pl.ds(base, 8), :] = x[k] + step
            s.seen[2 + i, t, pl.ds(base, 8), :] = y[k]
    outs = [[] for _ in range(6)]
    for k, t in enumerate(tiles):
        coverage = jnp.maximum(sums[1][k] + low[k] + high[k], 0.125)
        rc = inverse(coverage)
        s.rc[0, t, pl.ds(base, 8), :] = rc
        share = at(s.raw, 0, t, base) * rc
        rate = (0.5 * courant) * rc
        keep = share - 4.0 * rate
        c = [centre[f][k] for f in range(3)]
        e = [easts[f][k] for f in range(3)]
        w = [wests[f][k] for f in range(3)]
        north = [at(s.raw, 3 + f, t, base, 1) for f in range(3)]
        south = [at(s.raw, 3 + f, t, base, -1) for f in range(3)]
        flux = [(e[1] - w[1]) + (north[2] - south[2]), e[0] - w[0], north[0] - south[0]]
        outs[0].append(share)
        outs[1].append(share * at(s.raw, 1, t, base))
        outs[2].append(share * at(s.raw, 2, t, base))
        for f in range(3):
            around = (e[f] + w[f]) + (north[f] + south[f])
            outs[3 + f].append(keep * c[f] - rate * (flux[f] - around))
    for f in range(6):
        w = from_west(outs[f], west, lane)
        e = from_east(outs[f], east, lane)
        for k, t in enumerate(tiles):
            s.gath[3 * f, t, pl.ds(base, 8), :] = w[k]
            s.gath[3 * f + 1, t, pl.ds(base, 8), :] = outs[f][k]
            s.gath[3 * f + 2, t, pl.ds(base, 8), :] = e[k]


def stage_average(s, tiles, base):
    for t in tiles:
        weight = {}
        for dy in (-1, 0, 1):
            for dx in (-1, 0, 1):
                member = at(s.mk, 3 * (dy + 1) + dx + 1, t, base)
                weight[dy, dx] = (member, member * at(s.gath, 1 + dx, t, base, dy))
        cols = [weight[-1, d][1] + weight[0, d][1] + weight[1, d][1] for d in (-1, 0, 1)]
        total = cols[0] + cols[1] + cols[2]
        upper = weight[1, -1][1] + weight[1, 0][1] + weight[1, 1][1]
        lower = weight[-1, -1][1] + weight[-1, 0][1] + weight[-1, 1][1]
        sums = [cols[2] - cols[0], upper - lower, None, None, None]
        for f in range(5):
            for dy in (-1, 0, 1):
                for dx in (-1, 0, 1):
                    term = weight[dy, dx][0] * at(s.gath, 3 * (f + 1) + 1 + dx, t, base, dy)
                    sums[f] = term if sums[f] is None else sums[f] + term
        inv = inverse(jnp.maximum(total, 1e-3))
        for f in range(5):
            s.cent[f, t, pl.ds(base, 8), :] = sums[f] * inv


def stage_horizontal(s, tiles, west, east, base):
    lane = lane_index()
    results = [[at(s.cent, f, t, base) for t in tiles] for f in range(5)]
    w = [from_west(r, west, lane) for r in results]
    e = [from_east(r, east, lane) for r in results]
    for k, t in enumerate(tiles):
        x = [w[0][k] - 1.0, results[0][k], e[0][k] + 1.0]
        v = [w[1][k], results[1][k], e[1][k]]
        a = [[w[2 + f][k], results[2 + f][k], e[2 + f][k]] for f in range(3)]
        add3 = lambda p: p[0] + p[1] + p[2]
        dot3 = lambda p, q: p[0] * q[0] + p[1] * q[1] + p[2] * q[2]
        made = [add3(x), add3(v), dot3(x, x), dot3(x, v), dot3(v, v)]
        made += [add3(a[f]) for f in range(3)]
        made += [dot3(x, a[f]) for f in range(3)]
        made += [dot3(v, a[f]) for f in range(3)]
        for i, value in enumerate(made):
            s.horiz[i, t, pl.ds(base, 8), :] = value


def stage_slope(s, tiles, base):
    for t in tiles:
        rows = lambda i: [at(s.horiz, i, t, base, d) for d in (-1, 0, 1)]
        add3 = lambda p: p[0] + p[1] + p[2]
        u, v = at(s.cent, 0, t, base), at(s.cent, 1, t, base)
        hx, hv = rows(0), rows(1)
        sum_x, sum_y = add3(hx), add3(hv)
        sum_xx = add3(rows(2)) + 1.0
        sum_xy = add3(rows(3)) + (hx[2] - hx[0])
        sum_yy = add3(rows(4)) + (2.0 * (hv[2] - hv[0]) + 7.0)
        mean_x = sum_x - 9.0 * u
        mean_y = sum_y - 9.0 * v
        moment_xx = sum_xx - u * (sum_x + mean_x)
        moment_yy = sum_yy - v * (sum_y + mean_y)
        moment_xy = sum_xy - u * sum_y - v * mean_x
        inv = inverse(moment_xx * moment_yy - moment_xy * moment_xy)
        moment_xx = moment_xx * inv
        moment_yy = moment_yy * inv
        moment_xy = moment_xy * inv
        for f in range(3):
            average = at(s.cent, 2 + f, t, base)
            ha = rows(5 + f)
            sum_a = add3(ha)
            right_x = add3(rows(8 + f)) - u * sum_a - average * mean_x
            right_y = add3(rows(11 + f)) + (ha[2] - ha[0]) - v * sum_a - average * mean_y
            slope_x = moment_yy * right_x - moment_xy * right_y
            slope_y = moment_xx * right_y - moment_xy * right_x
            s.push[f, t, pl.ds(base, 8), :] = average - slope_x * u - slope_y * v
            s.push[3 + f, t, pl.ds(base, 8), :] = slope_x
            s.push[6 + f, t, pl.ds(base, 8), :] = slope_y


def stage_push(s, tiles, west, east, base):
    lane = lane_index()
    groups = [[[] for _ in range(3)] for _ in range(3)]
    for t in tiles:
        for dx in (-1, 0, 1):
            if dx:
                x, middle = at(s.seen, (dx + 1) // 2, t, base), at(s.seen, 2 + (dx + 1) // 2, t, base)
            else:
                x, middle = at(s.raw, 1, t, base), at(s.raw, 2, t, base)
            totals = [None] * 3
            for dy in (-1, 0, 1):
                y = middle + float(dy) if dy else middle
                member = at(s.mk, 3 * (dy + 1) + dx + 1, t, base, -dy)
                for f in range(3):
                    plane = at(s.push, f, t, base, -dy)
                    plane = plane + at(s.push, 3 + f, t, base, -dy) * x
                    plane = plane + at(s.push, 6 + f, t, base, -dy) * y
                    term = member * plane
                    totals[f] = term if totals[f] is None else totals[f] + term
            for f in range(3):
                groups[dx + 1][f].append(totals[f])
    results = []
    for f in range(3):
        low = from_east(groups[0][f], east, lane)
        high = from_west(groups[2][f], west, lane)
        results.append(
            [
                (groups[1][f][k] + low[k] + high[k]) * at(s.rc, 0, t, base)
                for k, t in enumerate(tiles)
            ]
        )
    return results


def start_all(copies):
    for copy in copies:
        copy.start()
    for copy in copies:
        copy.wait()


def strip_fields(state, cut, fraction, code, offset, rs, ls, limit):
    active = cut[rs, ls] > limit
    return [
        jnp.where(active, code[rs, ls], 16).astype(jnp.float32),
        jnp.where(active, fraction[rs, ls].astype(jnp.float32) * (1.0 / 1024.0), 1.0),
        jnp.where(active, offset[0, rs, ls], 0.0),
        jnp.where(active, offset[1, rs, ls], 0.0),
        state[0, rs, ls],
        state[1, rs, ls],
        state[2, rs, ls],
    ]


def pack_kernel(
    state_in, cut_in, fraction_in, code_in, flags_in, offset_in,
    s0, s1, own_rows, limit, state, cut, fraction, code, offset, flags, sem,
):
    rows, cols = cut_in.shape
    copies = [pltpu.make_async_copy(flags_in, flags, sem.at[2, 0])]
    for i in range(2):
        rs, to = pl.ds(i * (rows - 8), 8), pl.ds(8 * i, 8)
        pairs = [
            (cut_in.at[rs], cut.at[to]),
            (code_in.at[rs], code.at[to]),
            (fraction_in.at[rs], fraction.at[to]),
            (offset_in.at[:, rs], offset.at[:, to]),
            (state_in.at[:, rs], state.at[:, to]),
        ]
        copies += [pltpu.make_async_copy(a, b, sem.at[i, j]) for j, (a, b) in enumerate(pairs)]
    start_all(copies)
    even_y = lax.rem(lax.axis_index("ty"), 2) == 0
    for t in range(cols // LANES):
        ls = pl.ds(t * LANES, LANES)
        level = 1 - flags[0, t]
        limit[:, ls] = jnp.full((8, LANES), level, jnp.int32)
        made = []
        for i in range(2):
            got = strip_fields(state, cut, fraction, code, offset, pl.ds(8 * i, 8), ls, level)
            for f in range(FIELDS):
                own_rows[i, f, :, ls] = got[f]
            made.append(got)
        for f in range(FIELDS):
            top = made[0][f][0:4]
            bottom = made[1][f][4:8]
            s0[pl.ds(4 * f, 4), ls] = jnp.where(even_y, bottom, top)
            s1[pl.ds(4 * f, 4), ls] = jnp.where(even_y, top, bottom)


def in_vmem(value):
    return pltpu.with_memory_space_constraint(value, pltpu.VMEM)


def in_hbm(value):
    return pltpu.with_memory_space_constraint(value, pltpu.HBM)


VMEM_SPEC = pl.BlockSpec(memory_space=pltpu.VMEM)
SMEM_SPEC = pl.BlockSpec(memory_space=pltpu.SMEM)
HBM_SPEC = pl.BlockSpec(memory_space=pltpu.HBM)


def pack(*args):
    cols = args[1].shape[1]
    f32, i32 = jnp.float32, jnp.int32
    made = pl.pallas_call(
        pack_kernel,
        out_shape=(
            pltpu.VMEM((PACKED, cols), f32), pltpu.VMEM((PACKED, cols), f32),
            pltpu.VMEM((2, FIELDS, 8, cols), f32), pltpu.VMEM((8, cols), i32),
        ),
        in_specs=[HBM_SPEC] * 6,
        out_specs=[VMEM_SPEC] * 4,
        scratch_shapes=[
            pltpu.VMEM((3, 16, cols), f32),
            pltpu.VMEM((16, cols), i32),
            pltpu.VMEM((16, cols), i32),
            pltpu.VMEM((16, cols), i32),
            pltpu.VMEM((2, 16, cols), f32),
            pltpu.SMEM((1, cols // LANES), i32),
            pltpu.SemaphoreType.DMA((3, 5)),
        ],
        compiler_params=pltpu.CompilerParams(vmem_limit_bytes=2 * MIB),
        name="pack",
    )(*[in_hbm(a) for a in args])
    return [in_vmem(m) for m in made]


def first_kernel(
    state, cut, fraction, code, offset, limit, own_rows, p0, p1, own_cols, mk, raw, rc, seen, cent, gath, mix
):
    s = Fields(mk, raw, rc, seen, gath, cent, None, None)
    rows, cols = cut.shape
    ntile = cols // LANES
    tiles = list(range(ntile))
    west = [(t - 1) % ntile for t in tiles]
    east = [(t + 1) % ntile for t in tiles]

    even_x = lax.rem(lax.axis_index("tx"), 2) == 0
    ends = []
    for t in (0, ntile - 1):
        ls = pl.ds(t * LANES, LANES)
        ends.append(strip_fields(state, cut, fraction, code, offset, slice(None), ls, limit[0:1, ls]))
    half = lax.broadcasted_iota(jnp.int32, (rows, LANES), 1) < LANES // 2
    for f in range(FIELDS):
        turned = jnp.where(half, ends[0][f], ends[1][f]).T
        own_cols[0, f, :, :] = turned[0:8, :]
        own_cols[1, f, :, :] = turned[LANES - 8 :, :]
    for f in range(FIELDS):
        left = own_cols[0, f, 0:4, :]
        right = own_cols[1, f, 4:8, :]
        rs = pl.ds(4 * f, 4)
        p0[rs, 0:LANES] = jnp.where(even_x, right, left)
        p1[rs, 0:LANES] = jnp.where(even_x, left, right)
        for side in range(2):
            ls = pl.ds(side * (cols - LANES), LANES)
            first = 0 if side == 0 else LANES - 4
            near, far = own_rows[0, f, :, ls], own_rows[1, f, :, ls]
            for g, piece in ((1, near[0:4]), (2, near[4:8]), (3, far[0:4]), (4, far[4:8])):
                mix[side, g, rs, :] = pltpu.roll(piece, (4 * g - first) % LANES, 1)
    lane = lax.broadcasted_iota(jnp.int32, (PACKED, LANES), 1)
    parts = []
    for side in range(2):
        total = jnp.zeros((PACKED, LANES), jnp.float32)
        for g in range(1, 5):
            here = (lane >= 4 * g) & (lane < 4 * g + 4)
            total = jnp.where(here, mix[side, g, 0:PACKED, :], total)
        parts.append(total)
    p0[:, LANES:] = jnp.where(even_x, parts[1], parts[0])
    p1[:, LANES:] = jnp.where(even_x, parts[0], parts[1])

    def prepare(k, carry):
        src = pl.ds(pl.multiple_of(8 * k, 8), 8)
        dst = pl.ds(pl.multiple_of(8 * k + ORIGIN, 8), 8)
        for t in tiles:
            ls = pl.ds(t * LANES, LANES)
            active = cut[src, ls] > limit[:, ls]
            codes = jnp.where(active, code[src, ls], 16)
            kappa = jnp.where(active, fraction[src, ls].astype(jnp.float32) * (1.0 / 1024.0), 1.0)
            s.raw[0, t, dst, :] = kappa
            for i in range(2):
                s.raw[1 + i, t, dst, :] = jnp.where(active, offset[i, src, ls], 0.0)
            for f in range(3):
                s.raw[3 + f, t, dst, :] = state[f, src, ls]
            store_members(s.mk, codes, kappa, t, dst, plain_order)
        return carry

    def sweep(k, carry):
        stage_share(s, tiles, west, east, 8 * k + ORIGIN)
        return carry

    def sweep2(k, carry):
        stage_average(s, tiles, 8 * k + ORIGIN)
        return carry

    lax.fori_loop(0, rows // 8, prepare, 0)
    lax.fori_loop(0, rows // 8, sweep, 0)
    lax.fori_loop(0, rows // 8, sweep2, 0)


def second_kernel(mk, raw, rc, seen, cent, out, horiz, push):
    s = Fields(mk, raw, rc, seen, None, cent, horiz, push)
    ntile = mk.shape[1]
    count = out.shape[1] // 8
    tiles = list(range(ntile))
    west = [(t - 1) % ntile for t in tiles]
    east = [(t + 1) % ntile for t in tiles]

    def slopes(k, carry):
        stage_horizontal(s, tiles, west, east, 8 * k + ORIGIN)
        return carry

    def slopes2(k, carry):
        stage_slope(s, tiles, 8 * k + ORIGIN)
        return carry

    def spread(k, carry):
        made = stage_push(s, tiles, west, east, 8 * k + ORIGIN)
        for f in range(3):
            for t in tiles:
                out[f, pl.ds(pl.multiple_of(8 * k, 8), 8), pl.ds(t * LANES, LANES)] = made[f][t]
        return carry

    lax.fori_loop(0, count, slopes, 0)
    lax.fori_loop(0, count, slopes2, 0)
    lax.fori_loop(0, count, spread, 0)


def first_part(state, cut, fraction, code, offset, limit, own_rows):
    rows, cols = cut.shape
    ntile = cols // LANES
    f32 = jnp.float32
    mk, raw, rc, seen, _, cent, _, _ = Fields.shapes(ntile, rows + 16)
    gath = Fields.shapes(ntile + 1, rows + 24)[4]
    made = pl.pallas_call(
        first_kernel,
        out_shape=(
            pltpu.VMEM((PACKED, 2 * LANES), f32), pltpu.VMEM((PACKED, 2 * LANES), f32),
            pltpu.VMEM((2, FIELDS, 8, rows), f32), mk, raw, rc, seen, cent,
        ),
        in_specs=[VMEM_SPEC] * 7,
        out_specs=[VMEM_SPEC] * 8,
        scratch_shapes=[gath, pltpu.VMEM((2, 5, 32, LANES), f32)],
        compiler_params=pltpu.CompilerParams(vmem_limit_bytes=10 * MIB),
        cost_estimate=pl.CostEstimate(flops=30_000_000, transcendentals=0, bytes_accessed=1_000_000),
        name="first",
    )(state, cut, fraction, code, offset, limit, own_rows)
    return [in_vmem(m) for m in made]


def second_part(rows, *held):
    ntile = held[0].shape[1]
    *_, horiz, push = Fields.shapes(ntile + 1, rows + 24)
    return in_vmem(
        pl.pallas_call(
            second_kernel,
            out_shape=pltpu.VMEM((3, rows, ntile * LANES), jnp.float32),
            in_specs=[VMEM_SPEC] * 5,
            out_specs=VMEM_SPEC,
            scratch_shapes=[horiz, push],
            compiler_params=pltpu.CompilerParams(vmem_limit_bytes=12 * MIB),
            cost_estimate=pl.CostEstimate(flops=30_000_000, transcendentals=0, bytes_accessed=1_000_000),
            name="second",
        )(*held)
    )


swap_fields = (0, 1, 3, 2, 4, 6, 5)


def rim_kernel(h0, h1, c0, c1, own_rows, own_cols, base_ref, inner_out, out, wide, *rest):
    s = Fields(*rest[:8])
    turn, edge_c, edge_r, sem = rest[8:]
    _, rows, cols = out.shape
    ntile = cols // LANES
    inside = pl.ds(8, rows - 16)
    middle = pl.ds(LANES, cols - 2 * LANES)
    writes = [pltpu.make_async_copy(inner_out.at[:, inside, middle], out.at[:, inside, middle], sem.at[0])]
    writes[0].start()
    iy, ix = lax.axis_index("ty"), lax.axis_index("tx")
    even_y, even_x = lax.rem(iy, 2) == 0, lax.rem(ix, 2) == 0
    have_top, have_bottom = iy > 0, iy < lax.axis_size("ty") - 1
    have_left, have_right = ix > 0, ix < lax.axis_size("tx") - 1
    group = ntile + 1
    top, bottom, left, right = 0, group, 2 * group, 2 * group + 1
    zero4 = jnp.zeros((4, LANES), jnp.float32)
    halo = lambda even, a, b, have: jnp.where(have, jnp.where(even, a, b), zero4)
    for f in range(FIELDS):
        rs = pl.ds(4 * f, 4)
        for t in range(ntile):
            ls = pl.ds(t * LANES, LANES)
            wide[f, top + t, 0:4, :] = halo(even_y, h1[rs, ls], h0[rs, ls], have_top)
            wide[f, top + t, 4:12, :] = own_rows[0, f, :, ls]
            wide[f, bottom + t, 0:8, :] = own_rows[1, f, :, ls]
            wide[f, bottom + t, 8:12, :] = halo(even_y, h0[rs, ls], h1[rs, ls], have_bottom)
        fe = swap_fields[f]
        wide[fe, left, 0:4, :] = halo(even_x, c1[rs, 0:LANES], c0[rs, 0:LANES], have_left)
        wide[fe, left, 4:12, :] = own_cols[0, f, :, :]
        wide[fe, right, 0:8, :] = own_cols[1, f, :, :]
        wide[fe, right, 8:12, :] = halo(even_x, c0[rs, 0:LANES], c1[rs, 0:LANES], have_right)
    lane = lax.broadcasted_iota(jnp.int32, (PACKED, LANES), 1)
    none = jnp.zeros((PACKED, LANES), jnp.float32)
    a, b = c0[:, LANES:], c1[:, LANES:]
    from_left = jnp.where(have_left, jnp.where(even_x, b, a), none)
    from_right = jnp.where(have_right, jnp.where(even_x, a, b), none)
    for g in range(6):
        l = pltpu.roll(from_left, LANES - 4 - 4 * g, 1)
        r = pltpu.roll(from_right, (LANES - 4 * g) % LANES, 1)
        both = jnp.where(lane < 4, r, jnp.where(lane >= LANES - 4, l, 0.0))
        strip, first = ((top, 4 * g) if g < 3 else (bottom, 4 * (g - 3)))
        for f in range(FIELDS):
            wide[f, strip + ntile, first : first + 4, :] = both[4 * f : 4 * f + 4, :]

    tiles = list(range(2 * group + 2))
    west, east = list(tiles), list(tiles)
    for first in (top, bottom):
        for t in range(group):
            west[first + t] = first + (t - 1) % group
            east[first + t] = first + (t + 1) % group
    base = base_ref[0]
    for t in tiles:
        order = plain_order if t < left else swapped_order
        for r in range(2):
            rs = pl.ds(8 * r, 8)
            kappa = wide[1, t, rs, :]
            store_members(s.mk, wide[0, t, rs, :].astype(jnp.int32), kappa, t, rs, order)
            s.raw[0, t, rs, :] = kappa
            for f in range(2, FIELDS):
                s.raw[f - 1, t, rs, :] = wide[f, t, rs, :]
    def run(pick):
        w = [pick.index(west[t]) for t in pick]
        e = [pick.index(east[t]) for t in pick]
        stage_share(s, pick, w, e, base + 1)
        stage_share(s, pick, w, e, base + 9)
        stage_average(s, pick, base + 2)
        stage_horizontal(s, pick, w, e, base + 2)
        stage_slope(s, pick, base + 3)
        return stage_push(s, pick, w, e, base + 4)

    made = run([left, right])
    turn[...] = jnp.zeros_like(turn)
    for f in range(3):
        fe = (0, 2, 1)[f]
        turn[pl.ds(4 * f, 4), :] = made[fe][0][0:4]
        turn[pl.ds(16 + 4 * f, 4), :] = made[fe][1][0:4]
    back = turn[...].T
    lane = lax.broadcasted_iota(jnp.int32, (rows, LANES), 1)
    for f in range(3):
        left_cols = pltpu.roll(back, (LANES - 4 * f) % LANES, 1)
        right_cols = pltpu.roll(back, LANES - 4 - 16 - 4 * f, 1)
        edge_c[0, f] = jnp.where(lane < 4, left_cols, inner_out[f, :, 0:LANES])
        edge_c[1, f] = jnp.where(lane >= LANES - 4, right_cols, inner_out[f, :, cols - LANES :])
    for i, col in enumerate((0, cols - LANES)):
        writes.append(
            pltpu.make_async_copy(
                edge_c.at[i, :, inside], out.at[:, inside, pl.ds(col, LANES)], sem.at[1 + i]
            )
        )
        writes[-1].start()
    for i, (strip, row) in enumerate(((top, 0), (bottom, rows - 8))):
        made = run(list(range(strip, strip + group)))
        fresh = slice(0, 4) if i == 0 else slice(4, 8)
        kept = slice(4, 8) if i == 0 else slice(0, 4)
        rs = slice(row + kept.start, row + kept.stop)
        for f in range(3):
            for t in range(ntile):
                ls = pl.ds(t * LANES, LANES)
                edge_r[i, f, fresh, ls] = made[f][t][0:4]
                if t in (0, ntile - 1):
                    edge_r[i, f, kept, ls] = edge_c[min(t, 1), f, rs]
                else:
                    edge_r[i, f, kept, ls] = inner_out[f, rs, ls]
        writes.append(pltpu.make_async_copy(edge_r.at[i], out.at[:, pl.ds(row, 8)], sem.at[3 + i]))
        writes[-1].start()
    for copy in writes:
        copy.wait()


def rim(h0, h1, c0, c1, own_rows, own_cols, inner_out):
    _, rows, cols = inner_out.shape
    ntile = cols // LANES
    tiles = 2 * (ntile + 1) + 2
    f32 = jnp.float32
    return pl.pallas_call(
        rim_kernel,
        out_shape=pltpu.HBM((3, rows, cols), f32),
        in_specs=[VMEM_SPEC] * 6 + [SMEM_SPEC, VMEM_SPEC],
        out_specs=HBM_SPEC,
        scratch_shapes=[pltpu.VMEM((FIELDS, tiles + 1, 24, LANES), f32)]
        + Fields.shapes(tiles + 1, 24)
        + [
            pltpu.VMEM((LANES, LANES), f32),
            pltpu.VMEM((2, 3, rows, LANES), f32),
            pltpu.VMEM((2, 3, 8, cols), f32),
            pltpu.SemaphoreType.DMA((5,)),
        ],
        compiler_params=pltpu.CompilerParams(vmem_limit_bytes=16 * MIB),
        cost_estimate=pl.CostEstimate(flops=10_000_000, transcendentals=0, bytes_accessed=1_000_000),
        name="rim",
    )(h0, h1, c0, c1, own_rows, own_cols, jnp.zeros((1,), jnp.int32), inner_out)


def corner_kernel(h0, h1, p0, p1, q0, q1):
    iy, ix = lax.axis_index("ty"), lax.axis_index("tx")
    even_y, even_x = lax.rem(iy, 2) == 0, lax.rem(ix, 2) == 0
    have_top, have_bottom = iy > 0, iy < lax.axis_size("ty") - 1
    cols = h0.shape[1]
    lane = lax.broadcasted_iota(jnp.int32, (PACKED, LANES), 1)
    corners = []
    for first, ls in ((0, pl.ds(0, LANES)), (LANES - 4, pl.ds(cols - LANES, LANES))):
        a, b = h0[:, ls], h1[:, ls]
        above = jnp.where(have_top, jnp.where(even_y, b, a), 0.0)
        below = jnp.where(have_bottom, jnp.where(even_y, a, b), 0.0)
        above = pltpu.roll(above, (LANES - first) % LANES, 1)
        below = pltpu.roll(below, (20 + LANES - first) % LANES, 1)
        total = jnp.where(lane < 4, above, 0.0)
        corners.append(jnp.where((lane >= 20) & (lane < 24), below, total))
    left, right = corners
    q0[:, 0:LANES] = p0[:, 0:LANES]
    q1[:, 0:LANES] = p1[:, 0:LANES]
    q0[:, LANES:] = p0[:, LANES:] + jnp.where(even_x, right, left)
    q1[:, LANES:] = p1[:, LANES:] + jnp.where(even_x, left, right)


def with_corners(h0, h1, p0, p1):
    return pl.pallas_call(
        corner_kernel,
        out_shape=(pltpu.VMEM(p0.shape, jnp.float32), pltpu.VMEM(p1.shape, jnp.float32)),
        in_specs=[VMEM_SPEC] * 4,
        out_specs=[VMEM_SPEC] * 2,
        compiler_params=pltpu.CompilerParams(vmem_limit_bytes=2 * MIB),
        name="corner",
    )(h0, h1, p0, p1)


def body(state, cut_mask, fraction, neighbourhood, tile_flags, centroid_offset):
    args = (state, cut_mask, fraction, neighbourhood, tile_flags, centroid_offset)
    s0, s1, own_rows, limit = pack(*args)
    h0 = in_vmem(paired(s0, "ty", "tx", 0))
    h1 = in_vmem(paired(s1, "ty", "tx", 1))
    held = [in_vmem(a) for a in (state, cut_mask, fraction, neighbourhood, centroid_offset)]
    p0, p1, own_cols, *fields = first_part(*held, limit, own_rows)
    q0, q1 = with_corners(h0, h1, p0, p1)
    c0 = in_vmem(paired(q0, "tx", "ty", 0))
    c1 = in_vmem(paired(q1, "tx", "ty", 1))
    inner_out = second_part(state.shape[1], *fields)
    return rim(h0, h1, c0, c1, own_rows, own_cols, inner_out)


def solution(mesh):
    placed = (
        P(None, "ty", "tx"),
        P("ty", "tx"),
        P("ty", "tx"),
        P("ty", "tx"),
        P("ty", "tx"),
        P(None, "ty", "tx"),
    )
    return jax.shard_map(
        body, mesh=mesh, in_specs=placed, out_specs=P(None, "ty", "tx"), check_vma=False
    )
```
